32 devices in a mesh: section: 4 (over z), dom: 8 (over y, x, core).
Axes of the slice: x: 2, y: 2, z: 4, core: 2. Of those that a mesh axis runs over, the one named last changes fastest.
Arguments:
- layer_inputs: bfloat16 [4, 16384, 512], P('section', 'dom'), may hold values from -6 to 6
- adjacency: bfloat16 [128, 8, 128, 128], P('dom'), may hold values from -0.1875 to 0.1875
- columns: int32 [128, 8], P('dom'), may hold values from 0 to 127, as said below
- group_order: int32 [8, 4], P('dom'), may hold values from 0 to 3, each once within a row
- weights: bfloat16 [4, 512, 512], P('section'), may hold values from -0.25 to 0.25
Outputs:
- embeddings: bfloat16 [4, 16384, 512], P('section', 'dom')
The draws below stay inside these ranges and needn't reach their ends.
Inputs may be any that keep to these rules, and one draw needn't show every extreme that they name: `columns`: the tiles of a row block of part p name row blocks of parts p - 1, p and p + 1, counted modulo 8. `group_order`: each row is a permutation.
All inputs are finite; a program needn't handle non-finite values.
Results may differ from the reference program's by a relative error of at most 0.0095.
Values may be sent and summed in bfloat16 or wider, within the bound.
A program may use at most 64 MiB of HBM per device.

```python
import jax
import jax.numpy as jnp
from jax import lax

D = 512
BLOCK = 128
TILES = 8
GROUPS = 4
LAYERS = 4
PARTS_SIZE = 8
NODES = 16384
NBLK = 128
BPP = 16


def draw_columns(key, part):
    first_key, second_key = jax.random.split(jax.random.fold_in(key, 17))
    offsets = jax.random.randint(first_key, (NBLK, TILES), 0, 3) - 1
    inside = jax.random.randint(second_key, (NBLK, TILES), 0, BPP)
    owners = (jnp.arange(NBLK, dtype=jnp.int32) // BPP)[:, None]
    return ((owners + offsets) % PARTS_SIZE * BPP + inside).astype(jnp.int32)


def block_scale(key, dims, pieces, low, top_value):
    factor_of = 1.0
    for dim, blocks in pieces:
        draws = jax.random.uniform(jax.random.fold_in(jax.random.fold_in(key, 6), dim), (blocks,), jnp.float32, low / len(pieces), top_value / len(pieces))
        factor_of = factor_of * jnp.repeat(jnp.exp(draws), dims[dim] // blocks).reshape((-1,) + (1,) * (len(dims) - 1 - dim))
    return factor_of


def centred(own_key, dims, scale, bound, shards=(), held_as=jnp.bfloat16):
    factor_of = block_scale(own_key, dims, shards, -0.22, 0.18) if shards else 1.0
    array = jax.random.normal(own_key, dims, jnp.float32) * scale * factor_of
    return jnp.minimum(jnp.maximum(array, -bound), bound).astype(held_as)


def setup_inputs(seed: int = 0) -> dict:
    keys = jax.random.split(jax.random.key(seed), 6)
    layer_inputs = centred(keys[0], (LAYERS, NODES, D), 1.0, 6.0, ((0, 4), (1, 8)))
    adjacency = centred(keys[1], (NBLK, TILES, BLOCK, BLOCK), (TILES * BLOCK) ** -0.5, 0.1875, ((0, 8),))
    columns = draw_columns(jax.random.fold_in(keys[5], 71), 0)
    group_order = jax.vmap(lambda own: jax.random.permutation(own, GROUPS))(jax.random.split(keys[3], PARTS_SIZE)).reshape((PARTS_SIZE, GROUPS)).astype(jnp.int32)
    weights = centred(keys[4], (LAYERS, D, D), D ** -0.5, 0.25, ((0, 4),))
    return dict(layer_inputs=layer_inputs, adjacency=adjacency, columns=columns, group_order=group_order, weights=weights)


def reference(layer_inputs, adjacency, columns, group_order, weights):
    part_count = group_order.shape[0]
    blocks_part = adjacency.shape[0] // part_count
    blocks_group = blocks_part // GROUPS
    positions = jnp.arange(GROUPS, dtype=jnp.int32)
    matches = group_order[:, :, None] == positions[None, None, :]
    group_step = jnp.sum(jnp.where(matches, positions[None, :, None], 0), axis=1).astype(jnp.int32)
    block_ids = jnp.arange(NBLK, dtype=jnp.int32)
    block_step = group_step[block_ids // blocks_part, (block_ids % blocks_part) // blocks_group]
    fresh_mask = block_step[columns] <= block_step[:, None]
    tile_parts = adjacency.reshape(part_count, blocks_part, TILES, BLOCK, BLOCK)
    column_parts = columns.reshape(part_count, blocks_part, TILES)
    fresh_parts = fresh_mask.reshape(part_count, blocks_part, TILES)
    current = layer_inputs[0]
    results = []
    for layer_index in range(LAYERS):
        current_blocks = current.reshape(NBLK, BLOCK, D)
        stale_blocks = layer_inputs[layer_index].reshape(NBLK, BLOCK, D)

        def per_part(packed):
            tile_part, column_part, fresh_part = packed
            sources = jnp.where(fresh_part[:, :, None, None], current_blocks[column_part], stale_blocks[column_part])
            summed = jnp.einsum('rkij,rkjd->rid', tile_part.astype(jnp.float32), sources.astype(jnp.float32))
            return summed.astype(jnp.bfloat16)

        aggregate = lax.map(per_part, (tile_parts, column_parts, fresh_parts)).reshape(NODES, D)
        product = jnp.dot(aggregate, weights[layer_index], preferred_element_type=jnp.float32)
        current = (current.astype(jnp.float32) + jax.nn.relu(product)).astype(jnp.bfloat16)
        results.append(current)
    return jnp.stack(results)
```

```python
import functools

import jax
import jax.numpy as jnp
from jax import lax
from jax.experimental import pallas as pl
from jax.experimental.pallas import tpu as pltpu
from jax.sharding import PartitionSpec as P

MESH = pl.DeviceIdType.MESH
SPLIT = 2
AHEAD = 2


def relay_counts(blocks):
    return blocks * 7 // 16, blocks // 8


def pipeline_kernel(
    sections, parts, groups, columns, own_order, order_ref, x_ref, adj_hbm, w_ref, out_ref,
    table, position, order_land, near_order, order_send, order_recv, order_local,
    adj, src, mine, own_land, side_land, first_land, stored_land,
    adj_sem, partner_send, partner_recv, across_send, across_recv, z_send, z_recv, f_send, f_recv,
    over_send, over_recv, down_send, down_recv, sover_send, sover_recv, sdown_send, sdown_recv,
):
    s = lax.axis_index("section")
    d = lax.axis_index("dom")
    right, left = lax.rem(d + 1, parts), lax.rem(d + parts - 1, parts)
    blocks, side, width = x_ref.shape
    tiles = adj.shape[1]
    bg = blocks // groups
    fresh = 3 * blocks
    last = sections - 1
    odd = lax.rem(d, 2)
    partner = jnp.where(odd == 1, left, right)
    across = jnp.where(odd == 1, right, left)
    to_partner = jnp.where(odd == 1, 2 * blocks, 0)
    to_across = jnp.where(odd == 1, 0, 2 * blocks)
    from_across = jnp.where(odd == 1, 2 * blocks, 0)
    relayed, stored = relay_counts(blocks)
    direct = blocks - relayed
    low, mid = 1, 2
    half = side // SPLIT
    per_group = bg * SPLIT

    load_adj = pltpu.make_async_copy(adj_hbm, adj, adj_sem)
    load_adj.start()

    for k in range(groups):
        piece = x_ref[pl.ds(own_order[0, k] * bg, bg)]
        mine[k * bg:(k + 1) * bg] = piece
        src[blocks + k * bg:blocks + (k + 1) * bg] = piece

    barrier = pltpu.get_barrier_semaphore()

    def greet(there):
        pl.semaphore_signal(barrier, inc=1, device_id=there, device_id_type=MESH)

    peers = 2
    for neighbour in (left, right):
        greet({"dom": neighbour})
    for mask, there in (
        (s > 0, {"section": jnp.maximum(s - 1, 0)}),
        (s < last, {"section": jnp.minimum(s + 1, last)}),
        (s == 0, {"section": last, "dom": across}),
        (s == last, {"section": 0, "dom": across}),
        (s == 0, {"section": last}),
        (s == last, {"section": 0}),
        (s == low, {"section": mid, "dom": across}),
        (s == mid, {"section": low, "dom": across}),
    ):
        peers = peers + jnp.where(mask, 1, 0)

        @pl.when(mask)
        def _():
            greet(there)

    pl.semaphore_wait(barrier, peers)

    def order_copy(way):
        return pltpu.make_async_remote_copy(
            src_ref=order_ref,
            dst_ref=order_land.at[way],
            send_sem=order_send.at[way],
            recv_sem=order_recv.at[way],
            device_id={"dom": right if way == 0 else left},
            device_id_type=MESH,
        )

    def partner_copy(first, count):
        return pltpu.make_async_remote_copy(
            src_ref=mine.at[pl.ds(first, count)],
            dst_ref=src.at[pl.ds(to_partner + first, count)],
            send_sem=partner_send,
            recv_sem=partner_recv,
            device_id={"dom": partner},
            device_id_type=MESH,
        )

    def across_copy(n, first, count):
        return pltpu.make_async_remote_copy(
            src_ref=mine.at[pl.ds(first, count)],
            dst_ref=src.at[pl.ds(to_across + first, count)],
            send_sem=across_send.at[n],
            recv_sem=across_recv.at[n],
            device_id={"dom": across},
            device_id_type=MESH,
        )

    def over_copy(b):
        return pltpu.make_async_remote_copy(
            src_ref=mine.at[direct + b],
            dst_ref=first_land.at[b],
            send_sem=over_send.at[b],
            recv_sem=over_recv.at[b],
            device_id={"section": last, "dom": across},
            device_id_type=MESH,
        )

    def down_copy(b):
        return pltpu.make_async_remote_copy(
            src_ref=first_land.at[b],
            dst_ref=src.at[from_across + direct + b],
            send_sem=down_send.at[b],
            recv_sem=down_recv.at[b],
            device_id={"section": 0},
            device_id_type=MESH,
        )

    def stored_over_copy(b):
        return pltpu.make_async_remote_copy(
            src_ref=mine.at[blocks - stored + b],
            dst_ref=stored_land.at[b],
            send_sem=sover_send.at[b],
            recv_sem=sover_recv.at[b],
            device_id={"section": mid, "dom": across},
            device_id_type=MESH,
        )

    def stored_down_copy(b):
        return pltpu.make_async_remote_copy(
            src_ref=stored_land.at[b],
            dst_ref=src.at[from_across + blocks - stored + b],
            send_sem=sdown_send.at[b],
            recv_sem=sdown_recv.at[b],
            device_id={"section": low},
            device_id_type=MESH,
        )

    def up_copy(r, h):
        q = r * SPLIT + h
        return pltpu.make_async_remote_copy(
            src_ref=out_ref.at[r, pl.ds(h * half, half)],
            dst_ref=own_land.at[q],
            send_sem=z_send.at[q],
            recv_sem=z_recv.at[q],
            device_id={"section": jnp.minimum(s + 1, last)},
            device_id_type=MESH,
        )

    def up_wait(q):
        pltpu.make_async_remote_copy(
            src_ref=own_land.at[q],
            dst_ref=own_land.at[q],
            send_sem=z_send.at[q],
            recv_sem=z_recv.at[q],
            device_id={"section": jnp.minimum(s + 1, last)},
            device_id_type=MESH,
        ).wait_recv()

    def side_copy(way, q):
        return pltpu.make_async_remote_copy(
            src_ref=own_land.at[q],
            dst_ref=side_land.at[way, q],
            send_sem=f_send.at[way, q],
            recv_sem=f_recv.at[way, q],
            device_id={"dom": right if way == 0 else left},
            device_id_type=MESH,
        )

    def forward(q):
        up_wait(q)
        side_copy(0, q).start()
        side_copy(1, q).start()

    def stale_pieces(kept):
        return [(0, bg, bg), (1, 2 * bg, bg), (2, 3 * bg, bg - kept)]

    for way in range(2):
        order_copy(way).start()

    @pl.when(s == 0)
    def _():
        @pl.loop(0, relayed)
        def _(b):
            over_copy(b).start()

        across_copy(0, 0, direct).start()
        partner_copy(0, blocks).start()

    @pl.when(s == last)
    def _():
        @pl.loop(0, relayed)
        def _(b):
            over_copy(b).wait_recv()
            down_copy(b).start()

    @pl.when(s == low)
    def _():
        for n, first, count in stale_pieces(stored):
            across_copy(n, first, count).start()

    @pl.when(s > low)
    def _():
        for n, first, count in stale_pieces(0):
            across_copy(n, first, count).start()

    @pl.when(s > 0)
    def _():
        partner_copy(bg, blocks - bg).start()

    for way in range(2):
        order_copy(way).wait()
        local = pltpu.make_async_copy(
            order_land.at[way], near_order.at[way], order_local.at[way]
        )
        local.start()
        local.wait()

    for p in range(3):
        for g in range(groups):
            step = jnp.int32(0)
            for k in range(1, groups):
                held = own_order[0, k] if p == 1 else near_order[p // 2, 0, k]
                step = jnp.where(held == g, k, step)
            position[p * groups + g] = step

    later = s > 0

    @pl.loop(0, blocks)
    def _(r):
        k = r // bg
        row = own_order[0, k] * bg + r % bg
        for t in range(tiles):
            column = columns[t, row]
            relative = jnp.minimum(lax.rem(lax.div(column, blocks) - d + 1 + parts, parts), 2)
            inside = lax.rem(column, blocks)
            step = position[relative * groups + lax.div(inside, bg)]
            slot = relative * blocks + step * bg + lax.rem(inside, bg)
            table[r * tiles + t] = slot + jnp.where(later & (step <= k), fresh, 0)

    load_adj.wait()
    own_base = jnp.where(s > 0, fresh + blocks, blocks)

    @pl.when(s == low)
    def _():
        for n, first, count in stale_pieces(stored)[:2]:
            across_copy(n, first, count).wait_recv()

        @pl.loop(0, stored)
        def _(b):
            stored_over_copy(b).start()

    @pl.when(s == mid)
    def _():
        @pl.loop(0, stored)
        def _(b):
            stored_over_copy(b).wait_recv()
            stored_down_copy(b).start()

    for k in range(groups):
        lo, hi = k * bg, (k + 1) * bg
        plo, phi = lo * SPLIT, hi * SPLIT

        @pl.when(s > 0)
        def _():
            if k == 0:
                @pl.loop(0, per_group + AHEAD)
                def _(q):
                    forward(q)

            def as_blocks(pieces):
                return pieces.reshape(bg, side, width)

            src[fresh + blocks + lo:fresh + blocks + hi] = as_blocks(own_land[plo:phi])

            @pl.loop(plo, phi)
            def _(q):
                side_copy(0, q).wait_recv()
                side_copy(1, q).wait_recv()

            src[fresh + lo:fresh + hi] = as_blocks(side_land[0, plo:phi])
            src[fresh + 2 * blocks + lo:fresh + 2 * blocks + hi] = as_blocks(side_land[1, plo:phi])

        if k == 0:
            @pl.when(s == 0)
            def _():
                partner_copy(0, blocks).wait_recv()
                across_copy(0, 0, direct).wait_recv()

                @pl.loop(0, relayed)
                def _(b):
                    down_copy(b).wait_recv()

            @pl.when(s > 0)
            def _():
                partner_copy(bg, blocks - bg).wait_recv()

            @pl.when(s == low)
            def _():
                across_copy(*stale_pieces(stored)[2]).wait_recv()

                @pl.loop(0, stored)
                def _(b):
                    stored_down_copy(b).wait_recv()

            @pl.when(s > low)
            def _():
                for n, first, count in stale_pieces(0):
                    across_copy(n, first, count).wait_recv()

        @pl.loop(lo, hi)
        def _(r):
            row = own_order[0, k] * bg + (r - lo)
            a = jnp.concatenate([adj[row, t] for t in range(tiles)], axis=1)
            h = jnp.concatenate([src[table[r * tiles + t]] for t in range(tiles)], axis=0)
            agg = jnp.dot(a, h, preferred_element_type=jnp.float32).astype(jnp.bfloat16)
            product = jnp.dot(agg, w_ref[...], preferred_element_type=jnp.float32)
            before = src[own_base + r].astype(jnp.float32)
            out_ref[r] = (before + jnp.maximum(product, 0.0)).astype(jnp.bfloat16)

            @pl.when(s < last)
            def _():
                for h_ in range(SPLIT):
                    up_copy(r, h_).start()

            if k + 1 < groups:
                @pl.when(s > 0)
                def _():
                    forward(phi + AHEAD + (r - lo))

        if k + 1 < groups:
            more = per_group + (AHEAD if k + 2 < groups else 0)

            @pl.when(s > 0)
            def _():
                @pl.loop(phi + AHEAD + bg, phi + more)
                def _(q):
                    forward(q)

    @pl.when(s == 0)
    def _():
        partner_copy(0, blocks).wait_send()
        across_copy(0, 0, direct).wait_send()

        @pl.loop(0, relayed)
        def _(b):
            over_copy(b).wait_send()

    @pl.when(s == last)
    def _():
        @pl.loop(0, relayed)
        def _(b):
            down_copy(b).wait_send()

    @pl.when(s == low)
    def _():
        for n, first, count in stale_pieces(stored):
            across_copy(n, first, count).wait_send()

        @pl.loop(0, stored)
        def _(b):
            stored_over_copy(b).wait_send()

    @pl.when(s == mid)
    def _():
        @pl.loop(0, stored)
        def _(b):
            stored_down_copy(b).wait_send()

    @pl.when(s > low)
    def _():
        for n, first, count in stale_pieces(0):
            across_copy(n, first, count).wait_send()

    @pl.when(s > 0)
    def _():
        partner_copy(bg, blocks - bg).wait_send()

        @pl.loop(0, blocks * SPLIT)
        def _(q):
            side_copy(0, q).wait_send()
            side_copy(1, q).wait_send()

    @pl.when(s < last)
    def _():
        @pl.loop(0, blocks)
        def _(r):
            for h_ in range(SPLIT):
                up_copy(r, h_).wait_send()


def place_kernel(groups, order, h_hbm, out_hbm, held, in_sem, out_sem):
    bg = h_hbm.shape[0] // groups

    def load(k):
        rows = pl.ds(k * bg, bg)
        return pltpu.make_async_copy(h_hbm.at[rows], held.at[rows], in_sem.at[k])

    def store(k):
        return pltpu.make_async_copy(
            held.at[pl.ds(k * bg, bg)], out_hbm.at[pl.ds(order[k] * bg, bg)], out_sem.at[k]
        )

    for k in range(groups):
        load(k).start()
    for k in range(groups):
        load(k).wait()
        store(k).start()
    for k in range(groups):
        store(k).wait()


def on_device(sections, layer_inputs, adjacency, columns, group_order, weights):
    parts = lax.axis_size("dom")
    rows, width = layer_inputs.shape[1:]
    blocks, tiles, side = adjacency.shape[:3]
    groups = group_order.shape[1]
    relayed, stored = relay_counts(blocks)
    pieces = blocks * SPLIT
    dma = pltpu.SemaphoreType.DMA
    hidden = pl.pallas_call(
        functools.partial(pipeline_kernel, sections, parts, groups),
        out_shape=jax.ShapeDtypeStruct((blocks, side, width), jnp.bfloat16),
        in_specs=[
            pl.BlockSpec(memory_space=pltpu.SMEM),
            pl.BlockSpec(memory_space=pltpu.SMEM),
            pl.BlockSpec(memory_space=pltpu.VMEM),
            pl.BlockSpec(memory_space=pltpu.VMEM),
            pl.BlockSpec(memory_space=pl.ANY),
            pl.BlockSpec(memory_space=pltpu.VMEM),
        ],
        out_specs=pl.BlockSpec(memory_space=pltpu.VMEM),
        scratch_shapes=[
            pltpu.SMEM((blocks * tiles,), jnp.int32),
            pltpu.SMEM((3 * groups,), jnp.int32),
            pltpu.VMEM((2, 1, groups), jnp.int32),
            pltpu.SMEM((2, 1, groups), jnp.int32),
            dma((2,)),
            dma((2,)),
            dma((2,)),
            pltpu.VMEM(adjacency.shape, jnp.bfloat16),
            pltpu.VMEM((6 * blocks, side, width), jnp.bfloat16),
            pltpu.VMEM((blocks, side, width), jnp.bfloat16),
            pltpu.VMEM((pieces, side // SPLIT, width), jnp.bfloat16),
            pltpu.VMEM((2, pieces, side // SPLIT, width), jnp.bfloat16),
            pltpu.VMEM((relayed, side, width), jnp.bfloat16),
            pltpu.VMEM((stored, side, width), jnp.bfloat16),
            dma,
            dma,
            dma,
            dma((3,)),
            dma((3,)),
            dma((pieces,)),
            dma((pieces,)),
            dma((2, pieces)),
            dma((2, pieces)),
        ] + [dma((relayed,))] * 4 + [dma((stored,))] * 4,
        compiler_params=pltpu.CompilerParams(
            collective_id=0, has_side_effects=True, vmem_limit_bytes=56 * 2**20
        ),
    )(
        columns.T, group_order, group_order,
        layer_inputs.reshape(blocks, side, width), adjacency, weights[0],
    )

    placed = pl.pallas_call(
        functools.partial(place_kernel, groups),
        out_shape=jax.ShapeDtypeStruct((blocks, side, width), jnp.bfloat16),
        in_specs=[
            pl.BlockSpec(memory_space=pltpu.SMEM),
            pl.BlockSpec(memory_space=pl.ANY),
        ],
        out_specs=pl.BlockSpec(memory_space=pl.ANY),
        scratch_shapes=[
            pltpu.VMEM((blocks, side, width), jnp.bfloat16), dma((groups,)), dma((groups,)),
        ],
    )(group_order[0], hidden)
    return placed.reshape(1, rows, width)


def solution(mesh):
    in_specs = (
        P("section", "dom", None),
        P("dom", None, None, None),
        P("dom", None),
        P("dom", None),
        P("section", None, None),
    )
    return jax.shard_map(
        functools.partial(on_device, mesh.shape["section"]),
        mesh=mesh, in_specs=in_specs, out_specs=P("section", "dom", None), check_vma=False,
    )
```

```python
import functools

import jax
import jax.numpy as jnp
from jax import lax
from jax.experimental import pallas as pl
from jax.experimental.pallas import tpu as pltpu
from jax.sharding import PartitionSpec as P

MESH = pl.DeviceIdType.MESH
SPLIT = 2
AHEAD = 2


def relay_counts(blocks):
    return blocks * 7 // 16, blocks // 8


def pipeline_kernel(
    sections, parts, groups, columns_hbm, order_hbm, x_hbm, adj_hbm, w_hbm, out_ref,
    columns, own_order, order_ref, x_ref, w_ref, in_sem, table, position, order_land, near_order, order_send, order_recv, order_local,
    adj, src, mine, own_land, side_land, first_land, stored_land,
    adj_sem, partner_send, partner_recv, across_send, across_recv, z_send, z_recv, f_send, f_recv,
    over_send, over_recv, down_send, down_recv, sover_send, sover_recv, sdown_send, sdown_recv,
):
    s = lax.axis_index("section")
    d = lax.axis_index("dom")
    right, left = lax.rem(d + 1, parts), lax.rem(d + parts - 1, parts)
    blocks, side, width = x_ref.shape
    tiles = adj.shape[1]
    bg = blocks // groups
    fresh = 3 * blocks
    last = sections - 1
    odd = lax.rem(d, 2)
    partner = jnp.where(odd == 1, left, right)
    across = jnp.where(odd == 1, right, left)
    to_partner = jnp.where(odd == 1, 2 * blocks, 0)
    to_across = jnp.where(odd == 1, 0, 2 * blocks)
    from_across = jnp.where(odd == 1, 2 * blocks, 0)
    relayed, stored = relay_counts(blocks)
    direct = blocks - relayed
    low, mid = 1, 2
    half = side // SPLIT
    per_group = bg * SPLIT

    load_adj = pltpu.make_async_copy(adj_hbm, adj, adj_sem)
    loads = [
        pltpu.make_async_copy(there, here, in_sem.at[n])
        for n, (there, here) in enumerate((
            (order_hbm, own_order), (x_hbm, x_ref), (order_hbm, order_ref),
            (columns_hbm, columns), (w_hbm, w_ref),
        ))
    ]
    for load in loads:
        load.start()
    load_adj.start()
    loads[0].wait()
    loads[1].wait()

    for k in range(groups):
        piece = x_ref[pl.ds(own_order[0, k] * bg, bg)]
        mine[k * bg:(k + 1) * bg] = piece
        src[blocks + k * bg:blocks + (k + 1) * bg] = piece

    barrier = pltpu.get_barrier_semaphore()

    def greet(there):
        pl.semaphore_signal(barrier, inc=1, device_id=there, device_id_type=MESH)

    peers = 2
    for neighbour in (left, right):
        greet({"dom": neighbour})
    for mask, there in (
        (s > 0, {"section": jnp.maximum(s - 1, 0)}),
        (s < last, {"section": jnp.minimum(s + 1, last)}),
        (s == 0, {"section": last, "dom": across}),
        (s == last, {"section": 0, "dom": across}),
        (s == 0, {"section": last}),
        (s == last, {"section": 0}),
        (s == low, {"section": mid, "dom": across}),
        (s == mid, {"section": low, "dom": across}),
    ):
        peers = peers + jnp.where(mask, 1, 0)

        @pl.when(mask)
        def _():
            greet(there)

    pl.semaphore_wait(barrier, peers)

    def order_copy(way):
        return pltpu.make_async_remote_copy(
            src_ref=order_ref,
            dst_ref=order_land.at[way],
            send_sem=order_send.at[way],
            recv_sem=order_recv.at[way],
            device_id={"dom": right if way == 0 else left},
            device_id_type=MESH,
        )

    def partner_copy(first, count):
        return pltpu.make_async_remote_copy(
            src_ref=mine.at[pl.ds(first, count)],
            dst_ref=src.at[pl.ds(to_partner + first, count)],
            send_sem=partner_send,
            recv_sem=partner_recv,
            device_id={"dom": partner},
            device_id_type=MESH,
        )

    def across_copy(n, first, count):
        return pltpu.make_async_remote_copy(
            src_ref=mine.at[pl.ds(first, count)],
            dst_ref=src.at[pl.ds(to_across + first, count)],
            send_sem=across_send.at[n],
            recv_sem=across_recv.at[n],
            device_id={"dom": across},
            device_id_type=MESH,
        )

    def over_copy(b):
        return pltpu.make_async_remote_copy(
            src_ref=mine.at[direct + b],
            dst_ref=first_land.at[b],
            send_sem=over_send.at[b],
            recv_sem=over_recv.at[b],
            device_id={"section": last, "dom": across},
            device_id_type=MESH,
        )

    def down_copy(b):
        return pltpu.make_async_remote_copy(
            src_ref=first_land.at[b],
            dst_ref=src.at[from_across + direct + b],
            send_sem=down_send.at[b],
            recv_sem=down_recv.at[b],
            device_id={"section": 0},
            device_id_type=MESH,
        )

    def stored_over_copy(b):
        return pltpu.make_async_remote_copy(
            src_ref=mine.at[blocks - stored + b],
            dst_ref=stored_land.at[b],
            send_sem=sover_send.at[b],
            recv_sem=sover_recv.at[b],
            device_id={"section": mid, "dom": across},
            device_id_type=MESH,
        )

    def stored_down_copy(b):
        return pltpu.make_async_remote_copy(
            src_ref=stored_land.at[b],
            dst_ref=src.at[from_across + blocks - stored + b],
            send_sem=sdown_send.at[b],
            recv_sem=sdown_recv.at[b],
            device_id={"section": low},
            device_id_type=MESH,
        )

    def up_copy(r, h):
        q = r * SPLIT + h
        return pltpu.make_async_remote_copy(
            src_ref=out_ref.at[r, pl.ds(h * half, half)],
            dst_ref=own_land.at[q],
            send_sem=z_send.at[q],
            recv_sem=z_recv.at[q],
            device_id={"section": jnp.minimum(s + 1, last)},
            device_id_type=MESH,
        )

    def up_wait(q):
        pltpu.make_async_remote_copy(
            src_ref=own_land.at[q],
            dst_ref=own_land.at[q],
            send_sem=z_send.at[q],
            recv_sem=z_recv.at[q],
            device_id={"section": jnp.minimum(s + 1, last)},
            device_id_type=MESH,
        ).wait_recv()

    def side_copy(way, q):
        return pltpu.make_async_remote_copy(
            src_ref=own_land.at[q],
            dst_ref=side_land.at[way, q],
            send_sem=f_send.at[way, q],
            recv_sem=f_recv.at[way, q],
            device_id={"dom": right if way == 0 else left},
            device_id_type=MESH,
        )

    def forward(q):
        up_wait(q)
        side_copy(0, q).start()
        side_copy(1, q).start()

    def stale_pieces(kept):
        return [(0, bg, bg), (1, 2 * bg, bg), (2, 3 * bg, bg - kept)]

    loads[2].wait()
    for way in range(2):
        order_copy(way).start()

    @pl.when(s == 0)
    def _():
        @pl.loop(0, relayed)
        def _(b):
            over_copy(b).start()

        across_copy(0, 0, direct).start()
        partner_copy(0, blocks).start()

    @pl.when(s == last)
    def _():
        @pl.loop(0, relayed)
        def _(b):
            over_copy(b).wait_recv()
            down_copy(b).start()

    @pl.when(s == low)
    def _():
        for n, first, count in stale_pieces(stored):
            across_copy(n, first, count).start()

    @pl.when(s > low)
    def _():
        for n, first, count in stale_pieces(0):
            across_copy(n, first, count).start()

    @pl.when(s > 0)
    def _():
        partner_copy(bg, blocks - bg).start()

    for way in range(2):
        order_copy(way).wait()
        local = pltpu.make_async_copy(
            order_land.at[way], near_order.at[way], order_local.at[way]
        )
        local.start()
        local.wait()

    for p in range(3):
        for g in range(groups):
            step = jnp.int32(0)
            for k in range(1, groups):
                held = own_order[0, k] if p == 1 else near_order[p // 2, 0, k]
                step = jnp.where(held == g, k, step)
            position[p * groups + g] = step

    later = s > 0
    loads[3].wait()

    @pl.loop(0, blocks)
    def _(r):
        k = r // bg
        row = own_order[0, k] * bg + r % bg
        for t in range(tiles):
            column = columns[t, row]
            relative = jnp.minimum(lax.rem(lax.div(column, blocks) - d + 1 + parts, parts), 2)
            inside = lax.rem(column, blocks)
            step = position[relative * groups + lax.div(inside, bg)]
            slot = relative * blocks + step * bg + lax.rem(inside, bg)
            table[r * tiles + t] = slot + jnp.where(later & (step <= k), fresh, 0)

    load_adj.wait()
    loads[4].wait()
    own_base = jnp.where(s > 0, fresh + blocks, blocks)

    @pl.when(s == low)
    def _():
        for n, first, count in stale_pieces(stored)[:2]:
            across_copy(n, first, count).wait_recv()

        @pl.loop(0, stored)
        def _(b):
            stored_over_copy(b).start()

    @pl.when(s == mid)
    def _():
        @pl.loop(0, stored)
        def _(b):
            stored_over_copy(b).wait_recv()
            stored_down_copy(b).start()

    for k in range(groups):
        lo, hi = k * bg, (k + 1) * bg
        plo, phi = lo * SPLIT, hi * SPLIT

        @pl.when(s > 0)
        def _():
            if k == 0:
                @pl.loop(0, per_group + AHEAD)
                def _(q):
                    forward(q)

            def as_blocks(pieces):
                return pieces.reshape(bg, side, width)

            src[fresh + blocks + lo:fresh + blocks + hi] = as_blocks(own_land[plo:phi])

            @pl.loop(plo, phi)
            def _(q):
                side_copy(0, q).wait_recv()
                side_copy(1, q).wait_recv()

            src[fresh + lo:fresh + hi] = as_blocks(side_land[0, plo:phi])
            src[fresh + 2 * blocks + lo:fresh + 2 * blocks + hi] = as_blocks(side_land[1, plo:phi])

        if k == 0:
            @pl.when(s == 0)
            def _():
                partner_copy(0, blocks).wait_recv()
                across_copy(0, 0, direct).wait_recv()

                @pl.loop(0, relayed)
                def _(b):
                    down_copy(b).wait_recv()

            @pl.when(s > 0)
            def _():
                partner_copy(bg, blocks - bg).wait_recv()

            @pl.when(s == low)
            def _():
                across_copy(*stale_pieces(stored)[2]).wait_recv()

                @pl.loop(0, stored)
                def _(b):
                    stored_down_copy(b).wait_recv()

            @pl.when(s > low)
            def _():
                for n, first, count in stale_pieces(0):
                    across_copy(n, first, count).wait_recv()

        @pl.loop(lo, hi)
        def _(r):
            row = own_order[0, k] * bg + (r - lo)
            a = jnp.concatenate([adj[row, t] for t in range(tiles)], axis=1)
            h = jnp.concatenate([src[table[r * tiles + t]] for t in range(tiles)], axis=0)
            agg = jnp.dot(a, h, preferred_element_type=jnp.float32).astype(jnp.bfloat16)
            product = jnp.dot(agg, w_ref[...], preferred_element_type=jnp.float32)
            before = src[own_base + r].astype(jnp.float32)
            out_ref[r] = (before + jnp.maximum(product, 0.0)).astype(jnp.bfloat16)

            @pl.when(s < last)
            def _():
                for h_ in range(SPLIT):
                    up_copy(r, h_).start()

            if k + 1 < groups:
                @pl.when(s > 0)
                def _():
                    forward(phi + AHEAD + (r - lo))

        if k + 1 < groups:
            more = per_group + (AHEAD if k + 2 < groups else 0)

            @pl.when(s > 0)
            def _():
                @pl.loop(phi + AHEAD + bg, phi + more)
                def _(q):
                    forward(q)

    @pl.when(s == 0)
    def _():
        partner_copy(0, blocks).wait_send()
        across_copy(0, 0, direct).wait_send()

        @pl.loop(0, relayed)
        def _(b):
            over_copy(b).wait_send()

    @pl.when(s == last)
    def _():
        @pl.loop(0, relayed)
        def _(b):
            down_copy(b).wait_send()

    @pl.when(s == low)
    def _():
        for n, first, count in stale_pieces(stored):
            across_copy(n, first, count).wait_send()

        @pl.loop(0, stored)
        def _(b):
            stored_over_copy(b).wait_send()

    @pl.when(s == mid)
    def _():
        @pl.loop(0, stored)
        def _(b):
            stored_down_copy(b).wait_send()

    @pl.when(s > low)
    def _():
        for n, first, count in stale_pieces(0):
            across_copy(n, first, count).wait_send()

    @pl.when(s > 0)
    def _():
        partner_copy(bg, blocks - bg).wait_send()

        @pl.loop(0, blocks * SPLIT)
        def _(q):
            side_copy(0, q).wait_send()
            side_copy(1, q).wait_send()

    @pl.when(s < last)
    def _():
        @pl.loop(0, blocks)
        def _(r):
            for h_ in range(SPLIT):
                up_copy(r, h_).wait_send()


def place_kernel(groups, order, h_ref, out_hbm, out_sem):
    bg = h_ref.shape[0] // groups

    def store(k):
        return pltpu.make_async_copy(
            h_ref.at[pl.ds(k * bg, bg)], out_hbm.at[pl.ds(order[k] * bg, bg)], out_sem.at[k]
        )

    for k in range(groups):
        store(k).start()
    for k in range(groups):
        store(k).wait()


def on_device(sections, layer_inputs, adjacency, columns, group_order, weights):
    parts = lax.axis_size("dom")
    rows, width = layer_inputs.shape[1:]
    blocks, tiles, side = adjacency.shape[:3]
    groups = group_order.shape[1]
    relayed, stored = relay_counts(blocks)
    pieces = blocks * SPLIT
    dma = pltpu.SemaphoreType.DMA
    hidden = pl.pallas_call(
        functools.partial(pipeline_kernel, sections, parts, groups),
        out_shape=jax.ShapeDtypeStruct((blocks, side, width), jnp.bfloat16),
        in_specs=[
            pl.BlockSpec(memory_space=pltpu.HBM) for _ in range(5)
        ],
        out_specs=pl.BlockSpec(memory_space=pltpu.VMEM),
        scratch_shapes=[
            pltpu.SMEM((tiles, blocks), jnp.int32),
            pltpu.SMEM((1, groups), jnp.int32),
            pltpu.VMEM((1, groups), jnp.int32),
            pltpu.VMEM((blocks, side, width), jnp.bfloat16),
            pltpu.VMEM((width, width), jnp.bfloat16),
            dma((5,)),
            pltpu.SMEM((blocks * tiles,), jnp.int32),
            pltpu.SMEM((3 * groups,), jnp.int32),
            pltpu.VMEM((2, 1, groups), jnp.int32),
            pltpu.SMEM((2, 1, groups), jnp.int32),
            dma((2,)),
            dma((2,)),
            dma((2,)),
            pltpu.VMEM(adjacency.shape, jnp.bfloat16),
            pltpu.VMEM((6 * blocks, side, width), jnp.bfloat16),
            pltpu.VMEM((blocks, side, width), jnp.bfloat16),
            pltpu.VMEM((pieces, side // SPLIT, width), jnp.bfloat16),
            pltpu.VMEM((2, pieces, side // SPLIT, width), jnp.bfloat16),
            pltpu.VMEM((relayed, side, width), jnp.bfloat16),
            pltpu.VMEM((stored, side, width), jnp.bfloat16),
            dma,
            dma,
            dma,
            dma((3,)),
            dma((3,)),
            dma((pieces,)),
            dma((pieces,)),
            dma((2, pieces)),
            dma((2, pieces)),
        ] + [dma((relayed,))] * 4 + [dma((stored,))] * 4,
        compiler_params=pltpu.CompilerParams(
            collective_id=0, has_side_effects=True, vmem_limit_bytes=50 * 2**20
        ),
    )(
        *(pltpu.with_memory_space_constraint(array, pltpu.HBM) for array in (
            columns.T, group_order, layer_inputs.reshape(blocks, side, width),
            adjacency, weights[0],
        ))
    )

    placed = pl.pallas_call(
        functools.partial(place_kernel, groups),
        out_shape=jax.ShapeDtypeStruct((blocks, side, width), jnp.bfloat16),
        in_specs=[
            pl.BlockSpec(memory_space=pltpu.SMEM),
            pl.BlockSpec(memory_space=pltpu.VMEM),
        ],
        out_specs=pl.BlockSpec(memory_space=pl.ANY),
        scratch_shapes=[dma((groups,))],
        compiler_params=pltpu.CompilerParams(vmem_limit_bytes=4 * 2**20),
    )(group_order[0], hidden)
    return placed.reshape(1, rows, width)


def solution(mesh):
    in_specs = (
        P("section", "dom", None),
        P("dom", None, None, None),
        P("dom", None),
        P("dom", None),
        P("section", None, None),
    )
    return jax.shard_map(
        functools.partial(on_device, mesh.shape["section"]),
        mesh=mesh, in_specs=in_specs, out_specs=P("section", "dom", None), check_vma=False,
    )
```

```python
import functools

import jax
import jax.numpy as jnp
from jax import lax
from jax.experimental import pallas as pl
from jax.experimental.pallas import tpu as pltpu
from jax.sharding import PartitionSpec as P

MESH = pl.DeviceIdType.MESH
SPLIT = 2
AHEAD = 2
RUN = 2


def relay_counts(blocks):
    return blocks * 7 // 16, 3


def pipeline_kernel(
    sections, parts, groups, columns_hbm, order_hbm, x_hbm, adj_hbm, w_hbm, out_ref,
    columns, own_order, order_ref, x_ref, w_ref, in_sem, table, position, order_land, near_order, order_send, order_recv, order_local,
    adj, src, mine, own_land, side_land, first_land, stored_land,
    adj_sem, partner_send, partner_recv, across_send, across_recv, z_send, z_recv, f_send, f_recv,
    turn, over_send, over_recv, down_send, down_recv, sover_send, sover_recv, sdown_send, sdown_recv,
):
    s = lax.axis_index("section")
    d = lax.axis_index("dom")
    right, left = lax.rem(d + 1, parts), lax.rem(d + parts - 1, parts)
    blocks, side, width = x_ref.shape
    tiles = adj.shape[1]
    bg = blocks // groups
    fresh = 3 * blocks
    last = sections - 1
    odd = lax.rem(d, 2)
    partner = jnp.where(odd == 1, left, right)
    across = jnp.where(odd == 1, right, left)
    to_partner = jnp.where(odd == 1, 2 * blocks, 0)
    to_across = jnp.where(odd == 1, 0, 2 * blocks)
    from_across = jnp.where(odd == 1, 2 * blocks, 0)
    relayed, stored = relay_counts(blocks)
    direct = blocks - relayed
    low, mid = 1, 2
    half = side // SPLIT
    per_group = bg * SPLIT

    load_adj = pltpu.make_async_copy(adj_hbm, adj, adj_sem)
    loads = [
        pltpu.make_async_copy(there, here, in_sem.at[n])
        for n, (there, here) in enumerate((
            (order_hbm, own_order), (x_hbm, x_ref), (order_hbm, order_ref),
            (columns_hbm, columns), (w_hbm, w_ref),
        ))
    ]
    for load in loads:
        load.start()
    load_adj.start()
    barrier = pltpu.get_barrier_semaphore()

    def greet(there):
        pl.semaphore_signal(barrier, inc=1, device_id=there, device_id_type=MESH)

    peers = 2
    for neighbour in (left, right):
        greet({"dom": neighbour})
    for mask, there in (
        (s > 0, {"section": jnp.maximum(s - 1, 0)}),
        (s < last, {"section": jnp.minimum(s + 1, last)}),
        (s == 0, {"section": last, "dom": across}),
        (s == last, {"section": 0, "dom": across}),
        (s == 0, {"section": last}),
        (s == last, {"section": 0}),
        (s == low, {"section": mid, "dom": across}),
        (s == mid, {"section": low, "dom": across}),
    ):
        peers = peers + jnp.where(mask, 1, 0)

        @pl.when(mask)
        def _():
            greet(there)

    loads[0].wait()
    loads[1].wait()

    for k in range(groups):
        piece = x_ref[pl.ds(own_order[0, k] * bg, bg)]
        mine[k * bg:(k + 1) * bg] = piece
        src[blocks + k * bg:blocks + (k + 1) * bg] = piece

    pl.semaphore_wait(barrier, peers)

    def order_copy(way):
        return pltpu.make_async_remote_copy(
            src_ref=order_ref,
            dst_ref=order_land.at[way],
            send_sem=order_send.at[way],
            recv_sem=order_recv.at[way],
            device_id={"dom": right if way == 0 else left},
            device_id_type=MESH,
        )

    def partner_copy(first, count):
        return pltpu.make_async_remote_copy(
            src_ref=mine.at[pl.ds(first, count)],
            dst_ref=src.at[pl.ds(to_partner + first, count)],
            send_sem=partner_send,
            recv_sem=partner_recv,
            device_id={"dom": partner},
            device_id_type=MESH,
        )

    def across_copy(n, first, count):
        return pltpu.make_async_remote_copy(
            src_ref=mine.at[pl.ds(first, count)],
            dst_ref=src.at[pl.ds(to_across + first, count)],
            send_sem=across_send.at[n],
            recv_sem=across_recv.at[n],
            device_id={"dom": across},
            device_id_type=MESH,
        )

    def over_copy(b, h):
        return pltpu.make_async_remote_copy(
            src_ref=mine.at[direct + b, pl.ds(h * half, half)],
            dst_ref=first_land.at[b, pl.ds(h * half, half)],
            send_sem=over_send.at[b * SPLIT + h],
            recv_sem=over_recv.at[b * SPLIT + h],
            device_id={"section": last, "dom": across},
            device_id_type=MESH,
        )

    def down_copy(b, h):
        return pltpu.make_async_remote_copy(
            src_ref=first_land.at[b, pl.ds(h * half, half)],
            dst_ref=src.at[from_across + direct + b, pl.ds(h * half, half)],
            send_sem=down_send.at[b * SPLIT + h],
            recv_sem=down_recv.at[b * SPLIT + h],
            device_id={"section": 0},
            device_id_type=MESH,
        )

    def stored_over_copy(b):
        return pltpu.make_async_remote_copy(
            src_ref=mine.at[blocks - stored + b],
            dst_ref=stored_land.at[b],
            send_sem=sover_send.at[b],
            recv_sem=sover_recv.at[b],
            device_id={"section": mid, "dom": across},
            device_id_type=MESH,
        )

    def stored_down_copy(b):
        return pltpu.make_async_remote_copy(
            src_ref=stored_land.at[b],
            dst_ref=src.at[from_across + blocks - stored + b],
            send_sem=sdown_send.at[b],
            recv_sem=sdown_recv.at[b],
            device_id={"section": low},
            device_id_type=MESH,
        )

    def up_copy(r, h):
        q = r * SPLIT + h
        return pltpu.make_async_remote_copy(
            src_ref=out_ref.at[r, pl.ds(h * half, half)],
            dst_ref=own_land.at[q],
            send_sem=z_send.at[q],
            recv_sem=z_recv.at[q],
            device_id={"section": jnp.minimum(s + 1, last)},
            device_id_type=MESH,
        )

    def up_wait(q):
        pltpu.make_async_remote_copy(
            src_ref=own_land.at[q],
            dst_ref=own_land.at[q],
            send_sem=z_send.at[q],
            recv_sem=z_recv.at[q],
            device_id={"section": jnp.minimum(s + 1, last)},
            device_id_type=MESH,
        ).wait_recv()

    def side_copy(way, q):
        return pltpu.make_async_remote_copy(
            src_ref=own_land.at[q],
            dst_ref=side_land.at[way, q],
            send_sem=f_send.at[way, q],
            recv_sem=f_recv.at[way, q],
            device_id={"dom": right if way == 0 else left},
            device_id_type=MESH,
        )

    def forward(q):
        up_wait(q)
        side_copy(0, q).start()
        side_copy(1, q).start()

    def stale_pieces(kept):
        return [(0, bg, bg), (1, 2 * bg, bg), (2, 3 * bg, bg - kept)]

    loads[2].wait()
    for way in range(2):
        order_copy(way).start()

    def hand_over(n):
        pl.semaphore_signal(turn.at[n], inc=1, device_id={"dom": partner}, device_id_type=MESH)

    def each_relay(step):
        @pl.loop(0, relayed)
        def _(b):
            for h in range(SPLIT):
                step(b, h)

    @pl.when((s == 0) & (odd == 0))
    def _():
        each_relay(lambda b, h: over_copy(b, h).start())
        across_copy(0, 0, direct).start()

    @pl.when(s == 0)
    def _():
        partner_copy(0, blocks).start()

    @pl.when(s == last)
    def _():
        def pass_down(b, h):
            over_copy(b, h).wait_recv()
            down_copy(b, h).start()

        each_relay(pass_down)

    @pl.when((s == last) & (odd == 0))
    def _():
        hand_over(0)

    @pl.when((s == last) & (odd == 1))
    def _():
        pl.semaphore_wait(turn.at[0], 1)

    @pl.when(s == low)
    def _():
        for n, first, count in stale_pieces(stored):
            across_copy(n, first, count).start()

    @pl.when(s > low)
    def _():
        for n, first, count in stale_pieces(0):
            across_copy(n, first, count).start()

    @pl.when(s > 0)
    def _():
        partner_copy(bg, blocks - bg).start()

    for way in range(2):
        order_copy(way).wait()
        local = pltpu.make_async_copy(
            order_land.at[way], near_order.at[way], order_local.at[way]
        )
        local.start()
        local.wait()

    for p in range(3):
        for g in range(groups):
            step = jnp.int32(0)
            for k in range(1, groups):
                held = own_order[0, k] if p == 1 else near_order[p // 2, 0, k]
                step = jnp.where(held == g, k, step)
            position[p * groups + g] = step

    later = s > 0
    loads[3].wait()

    @pl.loop(0, blocks)
    def _(r):
        k = r // bg
        row = own_order[0, k] * bg + r % bg
        for t in range(tiles):
            column = columns[t, row]
            relative = jnp.minimum(lax.rem(lax.div(column, blocks) - d + 1 + parts, parts), 2)
            inside = lax.rem(column, blocks)
            step = position[relative * groups + lax.div(inside, bg)]
            slot = relative * blocks + step * bg + lax.rem(inside, bg)
            table[r * tiles + t] = slot + jnp.where(later & (step <= k), fresh, 0)

    load_adj.wait()
    loads[4].wait()
    own_base = jnp.where(s > 0, fresh + blocks, blocks)

    @pl.when((s == 0) & (odd == 0))
    def _():
        each_relay(lambda b, h: over_copy(b, h).wait_send())
        hand_over(0)
        across_copy(0, 0, direct).wait_send()
        hand_over(1)

    @pl.when((s == 0) & (odd == 1))
    def _():
        pl.semaphore_wait(turn.at[0], 1)
        each_relay(lambda b, h: over_copy(b, h).start())
        pl.semaphore_wait(turn.at[1], 1)
        across_copy(0, 0, direct).start()

    @pl.when(s == low)
    def _():
        for n, first, count in stale_pieces(stored)[:2]:
            across_copy(n, first, count).wait_recv()

        @pl.loop(0, stored)
        def _(b):
            stored_over_copy(b).start()

    @pl.when(s == mid)
    def _():
        @pl.loop(0, stored)
        def _(b):
            stored_over_copy(b).wait_recv()
            stored_down_copy(b).start()

    for k in range(groups):
        lo, hi = k * bg, (k + 1) * bg
        plo, phi = lo * SPLIT, hi * SPLIT

        @pl.when(s > 0)
        def _():
            if k == 0:
                @pl.loop(0, per_group + AHEAD)
                def _(q):
                    forward(q)

            def as_blocks(pieces):
                return pieces.reshape(bg, side, width)

            src[fresh + blocks + lo:fresh + blocks + hi] = as_blocks(own_land[plo:phi])

            @pl.loop(plo, phi)
            def _(q):
                side_copy(0, q).wait_recv()
                side_copy(1, q).wait_recv()

            src[fresh + lo:fresh + hi] = as_blocks(side_land[0, plo:phi])
            src[fresh + 2 * blocks + lo:fresh + 2 * blocks + hi] = as_blocks(side_land[1, plo:phi])

        if k == 0:
            @pl.when(s == 0)
            def _():
                partner_copy(0, blocks).wait_recv()
                across_copy(0, 0, direct).wait_recv()

                each_relay(lambda b, h: down_copy(b, h).wait_recv())

            @pl.when(s > 0)
            def _():
                partner_copy(bg, blocks - bg).wait_recv()

            @pl.when(s == low)
            def _():
                across_copy(*stale_pieces(stored)[2]).wait_recv()

                @pl.loop(0, stored)
                def _(b):
                    stored_down_copy(b).wait_recv()

            @pl.when(s > low)
            def _():
                for n, first, count in stale_pieces(0):
                    across_copy(n, first, count).wait_recv()

        @pl.loop(lo, hi)
        def _(r):
            if k == 1:
                @pl.when((s == 0) & (odd == 1) & (r == bg + RUN))
                def _():
                    pl.semaphore_wait(turn.at[2], 1)

            row = own_order[0, k] * bg + (r - lo)
            a = jnp.concatenate([adj[row, t] for t in range(tiles)], axis=1)
            h = jnp.concatenate([src[table[r * tiles + t]] for t in range(tiles)], axis=0)
            agg = jnp.dot(a, h, preferred_element_type=jnp.float32).astype(jnp.bfloat16)
            product = jnp.dot(agg, w_ref[...], preferred_element_type=jnp.float32)
            before = src[own_base + r].astype(jnp.float32)
            out_ref[r] = (before + jnp.maximum(product, 0.0)).astype(jnp.bfloat16)

            @pl.when(s < last)
            def _():
                for n in range(SPLIT):
                    up_copy(r, n).start()

            if k + 1 < groups:
                @pl.when(s > 0)
                def _():
                    forward(phi + AHEAD + (r - lo))

        if k == 0:
            @pl.when((s == 0) & (odd == 0))
            def _():
                @pl.loop(0, bg - 1)
                def _(r):
                    for h in range(SPLIT):
                        up_copy(r, h).wait_send()

                hand_over(2)

        if k + 1 < groups:
            more = per_group + (AHEAD if k + 2 < groups else 0)

            @pl.when(s > 0)
            def _():
                @pl.loop(phi + AHEAD + bg, phi + more)
                def _(q):
                    forward(q)

    @pl.when(s == 0)
    def _():
        partner_copy(0, blocks).wait_send()

    @pl.when((s == 0) & (odd == 1))
    def _():
        across_copy(0, 0, direct).wait_send()
        each_relay(lambda b, h: over_copy(b, h).wait_send())

    @pl.when(s == last)
    def _():
        each_relay(lambda b, h: down_copy(b, h).wait_send())

    @pl.when(s == low)
    def _():
        for n, first, count in stale_pieces(stored):
            across_copy(n, first, count).wait_send()

        @pl.loop(0, stored)
        def _(b):
            stored_over_copy(b).wait_send()

    @pl.when(s == mid)
    def _():
        @pl.loop(0, stored)
        def _(b):
            stored_down_copy(b).wait_send()

    @pl.when(s > low)
    def _():
        for n, first, count in stale_pieces(0):
            across_copy(n, first, count).wait_send()

    @pl.when(s > 0)
    def _():
        partner_copy(bg, blocks - bg).wait_send()

        @pl.loop(0, blocks * SPLIT)
        def _(q):
            side_copy(0, q).wait_send()
            side_copy(1, q).wait_send()

    waited = jnp.where((s == 0) & (odd == 0), bg - 1, 0)

    @pl.when(s < last)
    def _():
        @pl.loop(waited, blocks)
        def _(r):
            for h in range(SPLIT):
                up_copy(r, h).wait_send()


def place_kernel(groups, order, h_ref, out_hbm, out_sem):
    bg = h_ref.shape[0] // groups

    def store(k):
        return pltpu.make_async_copy(
            h_ref.at[pl.ds(k * bg, bg)], out_hbm.at[pl.ds(order[k] * bg, bg)], out_sem.at[k]
        )

    for k in range(groups):
        store(k).start()
    for k in range(groups):
        store(k).wait()


def on_device(sections, layer_inputs, adjacency, columns, group_order, weights):
    parts = lax.axis_size("dom")
    rows, width = layer_inputs.shape[1:]
    blocks, tiles, side = adjacency.shape[:3]
    groups = group_order.shape[1]
    relayed, stored = relay_counts(blocks)
    pieces = blocks * SPLIT
    dma = pltpu.SemaphoreType.DMA
    hidden = pl.pallas_call(
        functools.partial(pipeline_kernel, sections, parts, groups),
        out_shape=jax.ShapeDtypeStruct((blocks, side, width), jnp.bfloat16),
        in_specs=[
            pl.BlockSpec(memory_space=pltpu.HBM) for _ in range(5)
        ],
        out_specs=pl.BlockSpec(memory_space=pltpu.VMEM),
        scratch_shapes=[
            pltpu.SMEM((tiles, blocks), jnp.int32),
            pltpu.SMEM((1, groups), jnp.int32),
            pltpu.VMEM((1, groups), jnp.int32),
            pltpu.VMEM((blocks, side, width), jnp.bfloat16),
            pltpu.VMEM((width, width), jnp.bfloat16),
            dma((5,)),
            pltpu.SMEM((blocks * tiles,), jnp.int32),
            pltpu.SMEM((3 * groups,), jnp.int32),
            pltpu.VMEM((2, 1, groups), jnp.int32),
            pltpu.SMEM((2, 1, groups), jnp.int32),
            dma((2,)),
            dma((2,)),
            dma((2,)),
            pltpu.VMEM(adjacency.shape, jnp.bfloat16),
            pltpu.VMEM((6 * blocks, side, width), jnp.bfloat16),
            pltpu.VMEM((blocks, side, width), jnp.bfloat16),
            pltpu.VMEM((pieces, side // SPLIT, width), jnp.bfloat16),
            pltpu.VMEM((2, pieces, side // SPLIT, width), jnp.bfloat16),
            pltpu.VMEM((relayed, side, width), jnp.bfloat16),
            pltpu.VMEM((stored, side, width), jnp.bfloat16),
            dma,
            dma,
            dma,
            dma((3,)),
            dma((3,)),
            dma((pieces,)),
            dma((pieces,)),
            dma((2, pieces)),
            dma((2, pieces)),
        ] + [pltpu.SemaphoreType.REGULAR((3,))] + [dma((relayed * SPLIT,))] * 4 + [dma((stored,))] * 4,
        compiler_params=pltpu.CompilerParams(
            collective_id=0, has_side_effects=True, vmem_limit_bytes=50 * 2**20
        ),
    )(
        *(pltpu.with_memory_space_constraint(array, pltpu.HBM) for array in (
            columns.T, group_order, layer_inputs.reshape(blocks, side, width),
            adjacency, weights[0],
        ))
    )

    placed = pl.pallas_call(
        functools.partial(place_kernel, groups),
        out_shape=jax.ShapeDtypeStruct((blocks, side, width), jnp.bfloat16),
        in_specs=[
            pl.BlockSpec(memory_space=pltpu.SMEM),
            pl.BlockSpec(memory_space=pltpu.VMEM),
        ],
        out_specs=pl.BlockSpec(memory_space=pl.ANY),
        scratch_shapes=[dma((groups,))],
        compiler_params=pltpu.CompilerParams(vmem_limit_bytes=4 * 2**20),
    )(group_order[0], hidden)
    return placed.reshape(1, rows, width)


def solution(mesh):
    in_specs = (
        P("section", "dom", None),
        P("dom", None, None, None),
        P("dom", None),
        P("dom", None),
        P("section", None, None),
    )
    return jax.shard_map(
        functools.partial(on_device, mesh.shape["section"]),
        mesh=mesh, in_specs=in_specs, out_specs=P("section", "dom", None), check_vma=False,
    )
```

```python
import functools

import jax
import jax.numpy as jnp
from jax import lax
from jax.experimental import pallas as pl
from jax.experimental.pallas import tpu as pltpu
from jax.sharding import PartitionSpec as P

MESH = pl.DeviceIdType.MESH
SPLIT = 2
AHEAD = 2
FIRST_AHEAD = 0
RUN = 2
LAG = 4


def relay_counts(blocks):
    return blocks * 7 // 16, blocks * 5 // 8, blocks // 2


def pipeline_kernel(
    sections, parts, groups, columns_hbm, order_hbm, x_hbm, adj_hbm, w_hbm, out_ref,
    columns, own_order, order_ref, x_ref, w_ref, in_sem, table, position, order_land, near_order, order_send, order_recv, order_local,
    adj, src, mine, own_land, side_land, relay_in, relay_out, stored_in, stored_out,
    adj_sem, partner_send, partner_recv, across_send, across_recv, z_send, z_recv, f_send, f_recv,
    turn, lift_send, lift_recv, cross_send, cross_recv, down_send, down_recv,
    slift_send, slift_recv, scross_send, scross_recv, sdown_send, sdown_recv,
):
    s = lax.axis_index("section")
    d = lax.axis_index("dom")
    right, left = lax.rem(d + 1, parts), lax.rem(d + parts - 1, parts)
    blocks, side, width = x_ref.shape
    tiles = adj.shape[1]
    bg = blocks // groups
    fresh = 3 * blocks
    last = sections - 1
    odd = lax.rem(d, 2)
    partner = jnp.where(odd == 1, left, right)
    across = jnp.where(odd == 1, right, left)
    to_partner = jnp.where(odd == 1, 2 * blocks, 0)
    to_across = jnp.where(odd == 1, 0, 2 * blocks)
    from_across = jnp.where(odd == 1, 2 * blocks, 0)
    relayed, stored_low, stored_high = relay_counts(blocks)
    direct = blocks - relayed
    low = 1
    middle = (s > 0) & (s < last)
    stored = jnp.where(s == low, stored_low, stored_high)
    passed = jnp.where(s == low + 1, stored_low, stored_high)
    half = side // SPLIT
    aheads = [jnp.where((s == 1) & (odd == 0), FIRST_AHEAD, AHEAD)] + [AHEAD] * (groups - 2) + [0]
    per_group = bg * SPLIT

    load_adj = pltpu.make_async_copy(adj_hbm, adj, adj_sem)
    loads = [
        pltpu.make_async_copy(there, here, in_sem.at[n])
        for n, (there, here) in enumerate((
            (order_hbm, own_order), (x_hbm, x_ref), (order_hbm, order_ref),
            (columns_hbm, columns), (w_hbm, w_ref),
        ))
    ]
    for n in (2, 1, 0, 3, 4):
        loads[n].start()
    load_adj.start()
    barrier = pltpu.get_barrier_semaphore()

    def greet(there):
        pl.semaphore_signal(barrier, inc=1, device_id=there, device_id_type=MESH)

    peers = 2
    for neighbour in (left, right):
        greet({"dom": neighbour})
    for mask, there in (
        (s > 0, {"section": jnp.maximum(s - 1, 0)}),
        (s < last, {"section": jnp.minimum(s + 1, last)}),
    ):
        peers = peers + jnp.where(mask, 1, 0)

        @pl.when(mask)
        def _():
            greet(there)

    pl.semaphore_wait(barrier, peers)

    def order_copy(way):
        return pltpu.make_async_remote_copy(
            src_ref=order_ref,
            dst_ref=order_land.at[way],
            send_sem=order_send.at[way],
            recv_sem=order_recv.at[way],
            device_id={"dom": right if way == 0 else left},
            device_id_type=MESH,
        )

    def partner_copy(first, count, held=mine):
        return pltpu.make_async_remote_copy(
            src_ref=held.at[pl.ds(first, count)],
            dst_ref=src.at[pl.ds(to_partner + first, count)],
            send_sem=partner_send,
            recv_sem=partner_recv,
            device_id={"dom": partner},
            device_id_type=MESH,
        )

    def across_copy(n, first, count, held=mine):
        return pltpu.make_async_remote_copy(
            src_ref=held.at[pl.ds(first, count)],
            dst_ref=src.at[pl.ds(to_across + first, count)],
            send_sem=across_send.at[n],
            recv_sem=across_recv.at[n],
            device_id={"dom": across},
            device_id_type=MESH,
        )

    def relay_copy(held, landing, send, recv, there):
        return pltpu.make_async_remote_copy(
            src_ref=held, dst_ref=landing, send_sem=send, recv_sem=recv,
            device_id=there, device_id_type=MESH,
        )

    def lift(b, h):
        part, q = pl.ds(h * half, half), b * SPLIT + h
        return relay_copy(
            x_ref.at[direct + b, part], relay_in.at[b, part],
            lift_send.at[q], lift_recv.at[q], {"section": low},
        )

    def cross(b, h):
        part, q = pl.ds(h * half, half), b * SPLIT + h
        return relay_copy(
            relay_in.at[b, part], relay_out.at[b, part],
            cross_send.at[q], cross_recv.at[q], {"dom": across},
        )

    def down(b, h):
        part, q = pl.ds(h * half, half), b * SPLIT + h
        return relay_copy(
            relay_out.at[b, part], src.at[from_across + direct + b, part],
            down_send.at[q], down_recv.at[q], {"section": 0},
        )

    def stored_lift(b, count):
        return relay_copy(
            mine.at[blocks - count + b], stored_in.at[b],
            slift_send.at[b], slift_recv.at[b], {"section": jnp.minimum(s + 1, last)},
        )

    def stored_cross(b):
        return relay_copy(
            stored_in.at[b], stored_out.at[b],
            scross_send.at[b], scross_recv.at[b], {"dom": across},
        )

    def stored_down(b, count):
        return relay_copy(
            stored_out.at[b], src.at[from_across + blocks - count + b],
            sdown_send.at[b], sdown_recv.at[b], {"section": jnp.maximum(s - 1, 0)},
        )

    def up_copy(r, h):
        q = r * SPLIT + h
        return pltpu.make_async_remote_copy(
            src_ref=out_ref.at[r, pl.ds(h * half, half)],
            dst_ref=own_land.at[q],
            send_sem=z_send.at[q],
            recv_sem=z_recv.at[q],
            device_id={"section": jnp.minimum(s + 1, last)},
            device_id_type=MESH,
        )

    def up_wait(q):
        pltpu.make_async_remote_copy(
            src_ref=own_land.at[q],
            dst_ref=own_land.at[q],
            send_sem=z_send.at[q],
            recv_sem=z_recv.at[q],
            device_id={"section": jnp.minimum(s + 1, last)},
            device_id_type=MESH,
        ).wait_recv()

    def side_copy(way, q):
        return pltpu.make_async_remote_copy(
            src_ref=own_land.at[q],
            dst_ref=side_land.at[way, q],
            send_sem=f_send.at[way, q],
            recv_sem=f_recv.at[way, q],
            device_id={"dom": right if way == 0 else left},
            device_id_type=MESH,
        )

    def forward(q):
        up_wait(q)
        side_copy(0, q).start()
        side_copy(1, q).start()

    def stale_across(kept):
        return across_copy(0, bg, blocks - bg - kept)

    loads[2].wait()
    for way in range(2):
        order_copy(way).start()

    loads[1].wait()

    def hand_over(n):
        pl.semaphore_signal(turn.at[n], inc=1, device_id={"dom": partner}, device_id_type=MESH)

    def each_relay(step):
        @pl.loop(0, relayed)
        def _(b):
            for h in range(SPLIT):
                step(b, h)

    @pl.when((s == 0) & (odd == 0))
    def _():
        each_relay(lambda b, h: lift(b, h).start())
        across_copy(0, 0, direct, x_ref).start()

    @pl.when(s == 0)
    def _():
        partner_copy(0, blocks, x_ref).start()
        src[blocks:2 * blocks] = x_ref[...]

    loads[0].wait()

    @pl.when(s > 0)
    def _():
        for k in range(groups):
            piece = x_ref[pl.ds(own_order[0, k] * bg, bg)]
            mine[k * bg:(k + 1) * bg] = piece
            src[blocks + k * bg:blocks + (k + 1) * bg] = piece


    @pl.when(s > 0)
    def _():
        partner_copy(bg, blocks - bg).start()

    @pl.when(middle)
    def _():
        @pl.loop(0, stored)
        def _(b):
            stored_lift(b, stored).start()

    def pass_across(b, h):
        lift(b, h).wait_recv()
        cross(b, h).start()

    def pass_down(b, h):
        cross(b, h).wait_recv()
        down(b, h).start()

    @pl.when((s == low) & (odd == 0))
    def _():
        each_relay(pass_across)
        each_relay(pass_down)

    @pl.when((s == low) & (odd == 1))
    def _():
        @pl.loop(0, relayed - LAG // SPLIT)
        def _(b):
            for h in range(SPLIT):
                pass_down(b, h)

        @pl.loop(0, LAG // SPLIT)
        def _(b):
            for h in range(SPLIT):
                pass_across(b, h)
                pass_down(relayed - LAG // SPLIT + b, h)

        @pl.loop(LAG // SPLIT, relayed)
        def _(b):
            for h in range(SPLIT):
                pass_across(b, h)

    @pl.when(s == low)
    def _():
        stale_across(stored_low).start()

    @pl.when(s > low)
    def _():
        def stored_pass_across(b):
            stored_lift(b, passed).wait_recv()
            stored_cross(b).start()

        def stored_pass_down(b):
            stored_cross(b).wait_recv()
            stored_down(b, passed).start()

        stored_pass_across(0)
        stored_pass_across(1)

        @pl.loop(2, passed)
        def _(b):
            stored_pass_across(b)
            stored_pass_down(b - 2)

        @pl.when(s == last)
        def _():
            stale_across(0).start()

        @pl.when(s < last)
        def _():
            stale_across(stored_high).start()

        stored_pass_down(passed - 2)
        stored_pass_down(passed - 1)

    for way in range(2):
        order_copy(way).wait()
        local = pltpu.make_async_copy(
            order_land.at[way], near_order.at[way], order_local.at[way]
        )
        local.start()
        local.wait()

    for p in range(3):
        for g in range(groups):
            step = jnp.int32(0)
            for k in range(1, groups):
                held = own_order[0, k] if p == 1 else near_order[p // 2, 0, k]
                step = jnp.where(held == g, k, step)
            position[p * groups + g] = step

    later = s > 0
    loads[3].wait()

    @pl.loop(0, blocks)
    def _(r):
        k = r // bg
        row = own_order[0, k] * bg + r % bg
        for t in range(tiles):
            column = columns[t, row]
            relative = jnp.minimum(lax.rem(lax.div(column, blocks) - d + 1 + parts, parts), 2)
            inside = lax.rem(column, blocks)
            step = position[relative * groups + lax.div(inside, bg)]
            place = jnp.where(later, step * bg + lax.rem(inside, bg), inside)
            slot = relative * blocks + place
            table[r * tiles + t] = slot + jnp.where(later & (step <= k), fresh, 0)

    load_adj.wait()
    loads[4].wait()

    @pl.when((s == 0) & (odd == 0))
    def _():
        each_relay(lambda b, h: lift(b, h).wait_send())
        hand_over(0)
        across_copy(0, 0, direct, x_ref).wait_send()
        hand_over(1)

    @pl.when((s == 0) & (odd == 1))
    def _():
        pl.semaphore_wait(turn.at[0], 1)
        each_relay(lambda b, h: lift(b, h).start())
        pl.semaphore_wait(turn.at[1], 1)
        across_copy(0, 0, direct, x_ref).start()

    for k in range(groups):
        lo, hi = k * bg, (k + 1) * bg
        plo, phi = lo * SPLIT, hi * SPLIT

        @pl.when(s > 0)
        def _():
            if k == 0:
                @pl.loop(0, per_group + aheads[0])
                def _(q):
                    forward(q)

            def as_blocks(pieces):
                return pieces.reshape(bg, side, width)

            src[fresh + blocks + lo:fresh + blocks + hi] = as_blocks(own_land[plo:phi])

            @pl.loop(lo, hi)
            def _(r):
                for way in range(2):
                    for n in range(SPLIT):
                        side_copy(way, r * SPLIT + n).wait_recv()
                    block = side_land[way, pl.ds(r * SPLIT, SPLIT)]
                    src[fresh + 2 * way * blocks + r] = block.reshape(side, width)

        if k == 0:
            @pl.when(s == 0)
            def _():
                partner_copy(0, blocks, x_ref).wait_recv()
                across_copy(0, 0, direct, x_ref).wait_recv()

                each_relay(lambda b, h: down(b, h).wait_recv())

            @pl.when(s > 0)
            def _():
                partner_copy(bg, blocks - bg).wait_recv()

            @pl.when(middle)
            def _():
                @pl.when(s == low)
                def _():
                    stale_across(stored_low).wait_recv()

                @pl.when(s > low)
                def _():
                    stale_across(stored_high).wait_recv()

                @pl.loop(0, stored)
                def _(b):
                    stored_down(b, stored).wait_recv()

            @pl.when(s == last)
            def _():
                stale_across(0).wait_recv()

        def layer_row(r):
            row = own_order[0, k] * bg + (r - lo)
            a = jnp.concatenate([adj[row, t] for t in range(tiles)], axis=1)
            h = jnp.concatenate([src[table[r * tiles + t]] for t in range(tiles)], axis=0)
            agg = jnp.dot(a, h, preferred_element_type=jnp.float32).astype(jnp.bfloat16)
            product = jnp.dot(agg, w_ref[...], preferred_element_type=jnp.float32)
            own = jnp.where(later, fresh + blocks + r, blocks + row)
            before = src[own].astype(jnp.float32)
            out_ref[r] = (before + jnp.maximum(product, 0.0)).astype(jnp.bfloat16)

        closing = (s == last) if k == groups - 1 else (s < 0)
        if k == groups - 1:
            @pl.when(closing)
            def _():
                for r in range(lo, hi):
                    layer_row(r)

        @pl.loop(lo, jnp.where(closing, lo, hi))
        def _(r):
            if k == 1:
                @pl.when((s == 0) & (odd == 1) & (r == bg + RUN))
                def _():
                    pl.semaphore_wait(turn.at[2], 1)

            layer_row(r)

            @pl.when(s < last)
            def _():
                for n in range(SPLIT):
                    up_copy(r, n).start()

            if k + 1 < groups:
                @pl.when(s > 0)
                def _():
                    forward(phi + aheads[k] + (r - lo))

        if k == 0:
            @pl.when((s == 0) & (odd == 0))
            def _():
                @pl.loop(0, bg - 1)
                def _(r):
                    for h in range(SPLIT):
                        up_copy(r, h).wait_send()

                hand_over(2)

        if k + 1 < groups:
            more = per_group + aheads[k + 1]

            @pl.when(s > 0)
            def _():
                @pl.loop(phi + aheads[k] + bg, phi + more)
                def _(q):
                    forward(q)

    @pl.when(s == 0)
    def _():
        partner_copy(0, blocks, x_ref).wait_send()

    @pl.when((s == 0) & (odd == 1))
    def _():
        across_copy(0, 0, direct, x_ref).wait_send()
        each_relay(lambda b, h: lift(b, h).wait_send())

    @pl.when(s == low)
    def _():
        each_relay(lambda b, h: cross(b, h).wait_send())
        each_relay(lambda b, h: down(b, h).wait_send())

    @pl.when(middle)
    def _():
        @pl.when(s == low)
        def _():
            stale_across(stored_low).wait_send()

        @pl.when(s > low)
        def _():
            stale_across(stored_high).wait_send()

        @pl.loop(0, stored)
        def _(b):
            stored_lift(b, stored).wait_send()

    @pl.when(s == last)
    def _():
        stale_across(0).wait_send()

    @pl.when(s > low)
    def _():
        @pl.loop(0, passed)
        def _(b):
            stored_cross(b).wait_send()
            stored_down(b, passed).wait_send()

    @pl.when(s > 0)
    def _():
        partner_copy(bg, blocks - bg).wait_send()

        @pl.loop(0, blocks * SPLIT)
        def _(q):
            side_copy(0, q).wait_send()
            side_copy(1, q).wait_send()

    waited = jnp.where((s == 0) & (odd == 0), bg - 1, 0)

    @pl.when(s < last)
    def _():
        @pl.loop(waited, blocks)
        def _(r):
            for h in range(SPLIT):
                up_copy(r, h).wait_send()


def place_kernel(groups, order, h_ref, out_hbm, out_sem):
    bg = h_ref.shape[0] // groups

    def store(k):
        return pltpu.make_async_copy(
            h_ref.at[pl.ds(k * bg, bg)], out_hbm.at[pl.ds(order[k] * bg, bg)], out_sem.at[k]
        )

    for k in range(groups):
        store(k).start()
    for k in range(groups):
        store(k).wait()


def on_device(sections, layer_inputs, adjacency, columns, group_order, weights):
    parts = lax.axis_size("dom")
    rows, width = layer_inputs.shape[1:]
    blocks, tiles, side = adjacency.shape[:3]
    groups = group_order.shape[1]
    relayed, stored, _ = relay_counts(blocks)
    pieces = blocks * SPLIT
    dma = pltpu.SemaphoreType.DMA
    hidden = pl.pallas_call(
        functools.partial(pipeline_kernel, sections, parts, groups),
        out_shape=jax.ShapeDtypeStruct((blocks, side, width), jnp.bfloat16),
        in_specs=[
            pl.BlockSpec(memory_space=pltpu.HBM) for _ in range(5)
        ],
        out_specs=pl.BlockSpec(memory_space=pltpu.VMEM),
        scratch_shapes=[
            pltpu.SMEM((tiles, blocks), jnp.int32),
            pltpu.SMEM((1, groups), jnp.int32),
            pltpu.VMEM((1, groups), jnp.int32),
            pltpu.VMEM((blocks, side, width), jnp.bfloat16),
            pltpu.VMEM((width, width), jnp.bfloat16),
            dma((5,)),
            pltpu.SMEM((blocks * tiles,), jnp.int32),
            pltpu.SMEM((3 * groups,), jnp.int32),
            pltpu.VMEM((2, 1, groups), jnp.int32),
            pltpu.SMEM((2, 1, groups), jnp.int32),
            dma((2,)),
            dma((2,)),
            dma((2,)),
            pltpu.VMEM(adjacency.shape, jnp.bfloat16),
            pltpu.VMEM((6 * blocks, side, width), jnp.bfloat16),
            pltpu.VMEM((blocks, side, width), jnp.bfloat16),
            pltpu.VMEM((pieces, side // SPLIT, width), jnp.bfloat16),
            pltpu.VMEM((2, pieces, side // SPLIT, width), jnp.bfloat16),
            pltpu.VMEM((relayed, side, width), jnp.bfloat16),
            pltpu.VMEM((relayed, side, width), jnp.bfloat16),
            pltpu.VMEM((stored, side, width), jnp.bfloat16),
            pltpu.VMEM((stored, side, width), jnp.bfloat16),
            dma,
            dma,
            dma,
            dma((1,)),
            dma((1,)),
            dma((pieces,)),
            dma((pieces,)),
            dma((2, pieces)),
            dma((2, pieces)),
        ] + [pltpu.SemaphoreType.REGULAR((3,))]
        + [dma((relayed * SPLIT,))] * 6 + [dma((stored,))] * 6,
        compiler_params=pltpu.CompilerParams(
            collective_id=0, has_side_effects=True, vmem_limit_bytes=50 * 2**20
        ),
    )(
        *(pltpu.with_memory_space_constraint(array, pltpu.HBM) for array in (
            columns.T, group_order, layer_inputs.reshape(blocks, side, width),
            adjacency, weights[0],
        ))
    )

    placed = pl.pallas_call(
        functools.partial(place_kernel, groups),
        out_shape=jax.ShapeDtypeStruct((blocks, side, width), jnp.bfloat16),
        in_specs=[
            pl.BlockSpec(memory_space=pltpu.SMEM),
            pl.BlockSpec(memory_space=pltpu.VMEM),
        ],
        out_specs=pl.BlockSpec(memory_space=pl.ANY),
        scratch_shapes=[dma((groups,))],
        compiler_params=pltpu.CompilerParams(vmem_limit_bytes=4 * 2**20),
    )(group_order[0], hidden)
    return placed.reshape(1, rows, width)


def solution(mesh):
    in_specs = (
        P("section", "dom", None),
        P("dom", None, None, None),
        P("dom", None),
        P("dom", None),
        P("section", None, None),
    )
    return jax.shard_map(
        functools.partial(on_device, mesh.shape["section"]),
        mesh=mesh, in_specs=in_specs, out_specs=P("section", "dom", None), check_vma=False,
    )
```

```python
import functools

import jax
import jax.numpy as jnp
from jax import lax
from jax.experimental import pallas as pl
from jax.experimental.pallas import tpu as pltpu
from jax.sharding import PartitionSpec as P

MESH = pl.DeviceIdType.MESH
SPLIT = 2
AHEAD = 2
FIRST_AHEAD = 0
RUN = 2
LAG = 4


def relay_counts(blocks):
    return blocks * 7 // 16, blocks * 5 // 8, blocks // 2


def pipeline_kernel(
    sections, parts, groups, columns_hbm, order_hbm, x_hbm, adj_hbm, w_hbm, out_ref,
    columns, own_order, order_ref, x_ref, w_ref, in_sem, table, position, order_land, near_order, order_send, order_recv, order_local,
    adj, src, mine, own_land, side_land, relay_in, relay_out, stored_in, stored_out,
    adj_sem, partner_send, partner_recv, across_send, across_recv, z_send, z_recv, f_send, f_recv,
    turn, lift_send, lift_recv, cross_send, cross_recv, down_send, down_recv,
    slift_send, slift_recv, scross_send, scross_recv, sdown_send, sdown_recv,
):
    s = lax.axis_index("section")
    d = lax.axis_index("dom")
    right, left = lax.rem(d + 1, parts), lax.rem(d + parts - 1, parts)
    blocks, side, width = x_ref.shape
    tiles = adj.shape[1]
    bg = blocks // groups
    fresh = 3 * blocks
    last = sections - 1
    odd = lax.rem(d, 2)
    partner = jnp.where(odd == 1, left, right)
    across = jnp.where(odd == 1, right, left)
    to_partner = jnp.where(odd == 1, 2 * blocks, 0)
    to_across = jnp.where(odd == 1, 0, 2 * blocks)
    from_across = jnp.where(odd == 1, 2 * blocks, 0)
    relayed, stored_low, stored_high = relay_counts(blocks)
    direct = blocks - relayed
    low = 1
    middle = (s > 0) & (s < last)
    stored = jnp.where(s == low, stored_low, stored_high)
    passed = jnp.where(s == low + 1, stored_low, stored_high)
    half = side // SPLIT
    aheads = [jnp.where((s == 1) & (odd == 0), FIRST_AHEAD, AHEAD)] + [AHEAD] * (groups - 2) + [0]
    per_group = bg * SPLIT

    load_adj = pltpu.make_async_copy(adj_hbm, adj, adj_sem)
    loads = [
        pltpu.make_async_copy(there, here, in_sem.at[n])
        for n, (there, here) in enumerate((
            (order_hbm, own_order), (x_hbm, x_ref), (order_hbm, order_ref),
            (columns_hbm, columns), (w_hbm, w_ref),
        ))
    ]
    for n in (2, 1, 0, 3, 4):
        loads[n].start()
    load_adj.start()
    barrier = pltpu.get_barrier_semaphore()

    def greet(there):
        pl.semaphore_signal(barrier, inc=1, device_id=there, device_id_type=MESH)

    peers = 2
    for neighbour in (left, right):
        greet({"dom": neighbour})
    for mask, there in (
        (s > 0, {"section": jnp.maximum(s - 1, 0)}),
        (s < last, {"section": jnp.minimum(s + 1, last)}),
    ):
        peers = peers + jnp.where(mask, 1, 0)

        @pl.when(mask)
        def _():
            greet(there)

    pl.semaphore_wait(barrier, peers)

    def order_copy(way):
        return pltpu.make_async_remote_copy(
            src_ref=order_ref,
            dst_ref=order_land.at[way],
            send_sem=order_send.at[way],
            recv_sem=order_recv.at[way],
            device_id={"dom": right if way == 0 else left},
            device_id_type=MESH,
        )

    def partner_copy(first, count, held=mine):
        return pltpu.make_async_remote_copy(
            src_ref=held.at[pl.ds(first, count)],
            dst_ref=src.at[pl.ds(to_partner + first, count)],
            send_sem=partner_send,
            recv_sem=partner_recv,
            device_id={"dom": partner},
            device_id_type=MESH,
        )

    def across_copy(n, first, count, held=mine):
        return pltpu.make_async_remote_copy(
            src_ref=held.at[pl.ds(first, count)],
            dst_ref=src.at[pl.ds(to_across + first, count)],
            send_sem=across_send.at[n],
            recv_sem=across_recv.at[n],
            device_id={"dom": across},
            device_id_type=MESH,
        )

    def relay_copy(held, landing, send, recv, there):
        return pltpu.make_async_remote_copy(
            src_ref=held, dst_ref=landing, send_sem=send, recv_sem=recv,
            device_id=there, device_id_type=MESH,
        )

    def lifts():
        return relay_copy(
            x_ref.at[pl.ds(direct, relayed)], relay_in, lift_send, lift_recv.at[0],
            {"section": low},
        )

    def crosses():
        return relay_copy(relay_in, relay_out, cross_send, cross_recv.at[0], {"dom": across})

    def downs():
        return relay_copy(
            relay_out, src.at[pl.ds(from_across + direct, relayed)], down_send, down_recv,
            {"section": 0},
        )

    def lift(b, h):
        part, q = pl.ds(h * half, half), b * SPLIT + h
        return relay_copy(
            x_ref.at[direct + b, part], relay_in.at[b, part],
            lift_send, lift_recv.at[q], {"section": low},
        )

    def cross(b, h):
        part, q = pl.ds(h * half, half), b * SPLIT + h
        return relay_copy(
            relay_in.at[b, part], relay_out.at[b, part],
            cross_send, cross_recv.at[q], {"dom": across},
        )

    def down(b, h):
        part, q = pl.ds(h * half, half), b * SPLIT + h
        return relay_copy(
            relay_out.at[b, part], src.at[from_across + direct + b, part],
            down_send, down_recv, {"section": 0},
        )

    def stored_lift(b, count):
        return relay_copy(
            mine.at[blocks - count + b], stored_in.at[b],
            slift_send, slift_recv.at[b], {"section": jnp.minimum(s + 1, last)},
        )

    def stored_cross(b):
        return relay_copy(
            stored_in.at[b], stored_out.at[b],
            scross_send, scross_recv.at[b], {"dom": across},
        )

    def stored_down(b, count):
        return relay_copy(
            stored_out.at[b], src.at[from_across + blocks - count + b],
            sdown_send, sdown_recv, {"section": jnp.maximum(s - 1, 0)},
        )

    def stored_lifts(count):
        return relay_copy(
            mine.at[pl.ds(blocks - count, count)], stored_in.at[pl.ds(0, count)],
            slift_send, slift_recv.at[0], {"section": jnp.minimum(s + 1, last)},
        )

    def stored_crosses(count):
        return relay_copy(
            stored_in.at[pl.ds(0, count)], stored_out.at[pl.ds(0, count)],
            scross_send, scross_recv.at[0], {"dom": across},
        )

    def stored_downs(count):
        return relay_copy(
            stored_out.at[pl.ds(0, count)], src.at[pl.ds(from_across + blocks - count, count)],
            sdown_send, sdown_recv, {"section": jnp.maximum(s - 1, 0)},
        )

    def up_copy(r, h):
        q = r * SPLIT + h
        return pltpu.make_async_remote_copy(
            src_ref=out_ref.at[r, pl.ds(h * half, half)],
            dst_ref=own_land.at[q],
            send_sem=z_send.at[jnp.where(r < bg - 1, 0, 1)],
            recv_sem=z_recv.at[q],
            device_id={"section": jnp.minimum(s + 1, last)},
            device_id_type=MESH,
        )

    def up_sent(n):
        cut = (bg - 1) * SPLIT
        part = pl.ds(0, cut) if n == 0 else pl.ds(cut, blocks * SPLIT - cut)
        pltpu.make_async_remote_copy(
            src_ref=own_land.at[part], dst_ref=own_land.at[part],
            send_sem=z_send.at[n], recv_sem=z_recv.at[0],
            device_id={"section": jnp.minimum(s + 1, last)}, device_id_type=MESH,
        ).wait_send()

    def up_wait(q):
        pltpu.make_async_remote_copy(
            src_ref=own_land.at[q],
            dst_ref=own_land.at[q],
            send_sem=z_send.at[0],
            recv_sem=z_recv.at[q],
            device_id={"section": jnp.minimum(s + 1, last)},
            device_id_type=MESH,
        ).wait_recv()

    def side_copy(way, q):
        return pltpu.make_async_remote_copy(
            src_ref=own_land.at[q],
            dst_ref=side_land.at[way, q],
            send_sem=f_send.at[way],
            recv_sem=f_recv.at[way, q // SPLIT],
            device_id={"dom": right if way == 0 else left},
            device_id_type=MESH,
        )

    def side_block(way, r):
        part = pl.ds(r * SPLIT, SPLIT)
        return pltpu.make_async_remote_copy(
            src_ref=own_land.at[part],
            dst_ref=side_land.at[way, part],
            send_sem=f_send.at[way],
            recv_sem=f_recv.at[way, r],
            device_id={"dom": right if way == 0 else left},
            device_id_type=MESH,
        )

    def side_sent(way):
        pltpu.make_async_remote_copy(
            src_ref=own_land, dst_ref=side_land.at[way],
            send_sem=f_send.at[way], recv_sem=f_recv.at[way, 0],
            device_id={"dom": right if way == 0 else left}, device_id_type=MESH,
        ).wait_send()

    def forward(q):
        up_wait(q)
        side_copy(0, q).start()
        side_copy(1, q).start()

    def stale_across(kept):
        return across_copy(0, bg, blocks - bg - kept)

    loads[2].wait()
    for way in range(2):
        order_copy(way).start()

    loads[1].wait()

    def hand_over(n):
        pl.semaphore_signal(turn.at[n], inc=1, device_id={"dom": partner}, device_id_type=MESH)

    def each_relay(step):
        @pl.loop(0, relayed)
        def _(b):
            for h in range(SPLIT):
                step(b, h)

    @pl.when((s == 0) & (odd == 0))
    def _():
        each_relay(lambda b, h: lift(b, h).start())
        across_copy(0, 0, direct, x_ref).start()

    @pl.when(s == 0)
    def _():
        partner_copy(0, blocks, x_ref).start()
        src[blocks:2 * blocks] = x_ref[...]

    loads[0].wait()

    @pl.when(s > 0)
    def _():
        for k in range(groups):
            piece = x_ref[pl.ds(own_order[0, k] * bg, bg)]
            mine[k * bg:(k + 1) * bg] = piece
            src[blocks + k * bg:blocks + (k + 1) * bg] = piece


    @pl.when(s > 0)
    def _():
        partner_copy(bg, blocks - bg).start()

    @pl.when(middle)
    def _():
        @pl.loop(0, stored)
        def _(b):
            stored_lift(b, stored).start()

    def pass_across(b, h):
        lift(b, h).wait_recv()
        cross(b, h).start()

    def pass_down(b, h):
        cross(b, h).wait_recv()
        down(b, h).start()

    @pl.when((s == low) & (odd == 0))
    def _():
        each_relay(pass_across)
        each_relay(pass_down)

    @pl.when((s == low) & (odd == 1))
    def _():
        @pl.loop(0, relayed - LAG // SPLIT)
        def _(b):
            for h in range(SPLIT):
                pass_down(b, h)

        @pl.loop(0, LAG // SPLIT)
        def _(b):
            for h in range(SPLIT):
                pass_across(b, h)
                pass_down(relayed - LAG // SPLIT + b, h)

        @pl.loop(LAG // SPLIT, relayed)
        def _(b):
            for h in range(SPLIT):
                pass_across(b, h)

    @pl.when(s == low)
    def _():
        stale_across(stored_low).start()

    @pl.when(s > low)
    def _():
        def stored_pass_across(b):
            stored_lift(b, passed).wait_recv()
            stored_cross(b).start()

        def stored_pass_down(b):
            stored_cross(b).wait_recv()
            stored_down(b, passed).start()

        stored_pass_across(0)
        stored_pass_across(1)

        @pl.loop(2, passed)
        def _(b):
            stored_pass_across(b)
            stored_pass_down(b - 2)

        @pl.when(s == last)
        def _():
            stale_across(0).start()

        @pl.when(s < last)
        def _():
            stale_across(stored_high).start()

        stored_pass_down(passed - 2)
        stored_pass_down(passed - 1)

    for way in range(2):
        order_copy(way).wait()
        local = pltpu.make_async_copy(
            order_land.at[way], near_order.at[way], order_local.at[way]
        )
        local.start()
        local.wait()

    for p in range(3):
        for g in range(groups):
            step = jnp.int32(0)
            for k in range(1, groups):
                held = own_order[0, k] if p == 1 else near_order[p // 2, 0, k]
                step = jnp.where(held == g, k, step)
            position[p * groups + g] = step

    later = s > 0
    loads[3].wait()

    @pl.loop(0, blocks)
    def _(r):
        k = r // bg
        row = own_order[0, k] * bg + r % bg
        for t in range(tiles):
            column = columns[t, row]
            relative = jnp.minimum(lax.rem(lax.div(column, blocks) - d + 1 + parts, parts), 2)
            inside = lax.rem(column, blocks)
            step = position[relative * groups + lax.div(inside, bg)]
            place = jnp.where(later, step * bg + lax.rem(inside, bg), inside)
            slot = relative * blocks + place
            table[r * tiles + t] = slot + jnp.where(later & (step <= k), fresh, 0)

    load_adj.wait()
    loads[4].wait()

    @pl.when((s == 0) & (odd == 0))
    def _():
        lifts().wait_send()
        hand_over(0)
        across_copy(0, 0, direct, x_ref).wait_send()
        hand_over(1)

    @pl.when((s == 0) & (odd == 1))
    def _():
        pl.semaphore_wait(turn.at[0], 1)
        each_relay(lambda b, h: lift(b, h).start())
        pl.semaphore_wait(turn.at[1], 1)
        across_copy(0, 0, direct, x_ref).start()

    for k in range(groups):
        lo, hi = k * bg, (k + 1) * bg
        plo, phi = lo * SPLIT, hi * SPLIT

        @pl.when(s > 0)
        def _():
            if k == 0:
                @pl.loop(0, per_group + aheads[0])
                def _(q):
                    forward(q)

            def as_blocks(pieces):
                return pieces.reshape(bg, side, width)

            src[fresh + blocks + lo:fresh + blocks + hi] = as_blocks(own_land[plo:phi])

            @pl.loop(lo, hi)
            def _(r):
                for way in range(2):
                    side_block(way, r).wait_recv()
                    block = side_land[way, pl.ds(r * SPLIT, SPLIT)]
                    src[fresh + 2 * way * blocks + r] = block.reshape(side, width)

        if k == 0:
            @pl.when(s == 0)
            def _():
                partner_copy(0, blocks, x_ref).wait_recv()
                across_copy(0, 0, direct, x_ref).wait_recv()

                downs().wait_recv()

            @pl.when(s > 0)
            def _():
                partner_copy(bg, blocks - bg).wait_recv()

            @pl.when(middle)
            def _():
                @pl.when(s == low)
                def _():
                    stale_across(stored_low).wait_recv()
                    stored_downs(stored_low).wait_recv()

                @pl.when(s > low)
                def _():
                    stale_across(stored_high).wait_recv()
                    stored_downs(stored_high).wait_recv()

            @pl.when(s == last)
            def _():
                stale_across(0).wait_recv()

        def layer_row(r):
            row = own_order[0, k] * bg + (r - lo)
            a = jnp.concatenate([adj[row, t] for t in range(tiles)], axis=1)
            h = jnp.concatenate([src[table[r * tiles + t]] for t in range(tiles)], axis=0)
            agg = jnp.dot(a, h, preferred_element_type=jnp.float32).astype(jnp.bfloat16)
            product = jnp.dot(agg, w_ref[...], preferred_element_type=jnp.float32)
            own = jnp.where(later, fresh + blocks + r, blocks + row)
            before = src[own].astype(jnp.float32)
            out_ref[r] = (before + jnp.maximum(product, 0.0)).astype(jnp.bfloat16)

        closing = (s == last) if k == groups - 1 else (s < 0)
        if k == groups - 1:
            @pl.when(closing)
            def _():
                for r in range(lo, hi):
                    layer_row(r)

        @pl.loop(lo, jnp.where(closing, lo, hi))
        def _(r):
            if k == 1:
                @pl.when((s == 0) & (odd == 1) & (r == bg + RUN))
                def _():
                    pl.semaphore_wait(turn.at[2], 1)

            layer_row(r)

            @pl.when(s < last)
            def _():
                for n in range(SPLIT):
                    up_copy(r, n).start()

            if k + 1 < groups:
                @pl.when(s > 0)
                def _():
                    forward(phi + aheads[k] + (r - lo))

        if k == 0:
            @pl.when((s == 0) & (odd == 0))
            def _():
                up_sent(0)
                hand_over(2)

        if k + 1 < groups:
            more = per_group + aheads[k + 1]

            @pl.when(s > 0)
            def _():
                @pl.loop(phi + aheads[k] + bg, phi + more)
                def _(q):
                    forward(q)

    @pl.when(s == 0)
    def _():
        partner_copy(0, blocks, x_ref).wait_send()

    @pl.when((s == 0) & (odd == 1))
    def _():
        across_copy(0, 0, direct, x_ref).wait_send()
        lifts().wait_send()

    @pl.when(s == low)
    def _():
        crosses().wait_send()
        downs().wait_send()

    @pl.when(s == low)
    def _():
        stale_across(stored_low).wait_send()
        stored_lifts(stored_low).wait_send()

    @pl.when((s > low) & (s < last))
    def _():
        stale_across(stored_high).wait_send()
        stored_lifts(stored_high).wait_send()

    @pl.when(s == last)
    def _():
        stale_across(0).wait_send()

    for mask, count in ((s == low + 1, stored_low), (s > low + 1, stored_high)):
        @pl.when(mask)
        def _():
            stored_crosses(count).wait_send()
            stored_downs(count).wait_send()

    @pl.when(s > 0)
    def _():
        partner_copy(bg, blocks - bg).wait_send()
        for way in range(2):
            side_sent(way)

    @pl.when((s < last) & ((s > 0) | (odd == 1)))
    def _():
        up_sent(0)

    @pl.when(s < last)
    def _():
        up_sent(1)


def place_kernel(groups, order, h_ref, out_hbm, out_sem):
    bg = h_ref.shape[0] // groups

    def store(k):
        return pltpu.make_async_copy(
            h_ref.at[pl.ds(k * bg, bg)], out_hbm.at[pl.ds(order[k] * bg, bg)], out_sem.at[k]
        )

    for k in range(groups):
        store(k).start()
    for k in range(groups):
        store(k).wait()


def on_device(sections, layer_inputs, adjacency, columns, group_order, weights):
    parts = lax.axis_size("dom")
    rows, width = layer_inputs.shape[1:]
    blocks, tiles, side = adjacency.shape[:3]
    groups = group_order.shape[1]
    relayed, stored, _ = relay_counts(blocks)
    pieces = blocks * SPLIT
    dma = pltpu.SemaphoreType.DMA
    hidden = pl.pallas_call(
        functools.partial(pipeline_kernel, sections, parts, groups),
        out_shape=jax.ShapeDtypeStruct((blocks, side, width), jnp.bfloat16),
        in_specs=[
            pl.BlockSpec(memory_space=pltpu.HBM) for _ in range(5)
        ],
        out_specs=pl.BlockSpec(memory_space=pltpu.VMEM),
        scratch_shapes=[
            pltpu.SMEM((tiles, blocks), jnp.int32),
            pltpu.SMEM((1, groups), jnp.int32),
            pltpu.VMEM((1, groups), jnp.int32),
            pltpu.VMEM((blocks, side, width), jnp.bfloat16),
            pltpu.VMEM((width, width), jnp.bfloat16),
            dma((5,)),
            pltpu.SMEM((blocks * tiles,), jnp.int32),
            pltpu.SMEM((3 * groups,), jnp.int32),
            pltpu.VMEM((2, 1, groups), jnp.int32),
            pltpu.SMEM((2, 1, groups), jnp.int32),
            dma((2,)),
            dma((2,)),
            dma((2,)),
            pltpu.VMEM(adjacency.shape, jnp.bfloat16),
            pltpu.VMEM((6 * blocks, side, width), jnp.bfloat16),
            pltpu.VMEM((blocks, side, width), jnp.bfloat16),
            pltpu.VMEM((pieces, side // SPLIT, width), jnp.bfloat16),
            pltpu.VMEM((2, pieces, side // SPLIT, width), jnp.bfloat16),
            pltpu.VMEM((relayed, side, width), jnp.bfloat16),
            pltpu.VMEM((relayed, side, width), jnp.bfloat16),
            pltpu.VMEM((stored, side, width), jnp.bfloat16),
            pltpu.VMEM((stored, side, width), jnp.bfloat16),
            dma,
            dma,
            dma,
            dma((1,)),
            dma((1,)),
            dma((2,)),
            dma((pieces,)),
            dma((2,)),
            dma((2, blocks)),
        ] + [pltpu.SemaphoreType.REGULAR((3,))]
        + [dma, dma((relayed * SPLIT,))] * 2 + [dma, dma] + [dma, dma((stored,))] * 2 + [dma, dma],
        compiler_params=pltpu.CompilerParams(
            collective_id=0, has_side_effects=True, vmem_limit_bytes=50 * 2**20
        ),
    )(
        *(pltpu.with_memory_space_constraint(array, pltpu.HBM) for array in (
            columns.T, group_order, layer_inputs.reshape(blocks, side, width),
            adjacency, weights[0],
        ))
    )

    placed = pl.pallas_call(
        functools.partial(place_kernel, groups),
        out_shape=jax.ShapeDtypeStruct((blocks, side, width), jnp.bfloat16),
        in_specs=[
            pl.BlockSpec(memory_space=pltpu.SMEM),
            pl.BlockSpec(memory_space=pltpu.VMEM),
        ],
        out_specs=pl.BlockSpec(memory_space=pl.ANY),
        scratch_shapes=[dma((groups,))],
        compiler_params=pltpu.CompilerParams(vmem_limit_bytes=4 * 2**20),
    )(group_order[0], hidden)
    return placed.reshape(1, rows, width)


def solution(mesh):
    in_specs = (
        P("section", "dom", None),
        P("dom", None, None, None),
        P("dom", None),
        P("dom", None),
        P("section", None, None),
    )
    return jax.shard_map(
        functools.partial(on_device, mesh.shape["section"]),
        mesh=mesh, in_specs=in_specs, out_specs=P("section", "dom", None), check_vma=False,
    )
```

```python
import functools

import jax
import jax.numpy as jnp
from jax import lax
from jax.experimental import pallas as pl
from jax.experimental.pallas import tpu as pltpu
from jax.sharding import PartitionSpec as P

MESH = pl.DeviceIdType.MESH
SPLIT = 2
UP = 4
AHEAD = 4
FIRST_AHEAD = 0
RUN = 2
LAG = 4


def relay_counts(blocks):
    return blocks * 7 // 16, blocks * 5 // 8, blocks // 2


def pipeline_kernel(
    sections, parts, groups, columns_hbm, order_hbm, x_hbm, adj_hbm, w_hbm, out_ref,
    columns, own_order, order_ref, x_ref, w_ref, in_sem, table, position, order_land, near_order, order_send, order_recv, order_local,
    adj, src, mine, own_land, side_land, relay_in, relay_out, stored_in, stored_out,
    adj_sem, partner_send, partner_recv, across_send, across_recv, z_send, z_recv, f_send, f_recv,
    turn, lift_send, lift_recv, cross_send, cross_recv, down_send, down_recv,
    slift_send, slift_recv, scross_send, scross_recv, sdown_send, sdown_recv,
):
    s = lax.axis_index("section")
    d = lax.axis_index("dom")
    right, left = lax.rem(d + 1, parts), lax.rem(d + parts - 1, parts)
    blocks, side, width = x_ref.shape
    tiles = adj.shape[1]
    bg = blocks // groups
    fresh = 3 * blocks
    last = sections - 1
    odd = lax.rem(d, 2)
    partner = jnp.where(odd == 1, left, right)
    across = jnp.where(odd == 1, right, left)
    to_partner = jnp.where(odd == 1, 2 * blocks, 0)
    to_across = jnp.where(odd == 1, 0, 2 * blocks)
    from_across = jnp.where(odd == 1, 2 * blocks, 0)
    relayed, stored_low, stored_high = relay_counts(blocks)
    direct = blocks - relayed
    low = 1
    middle = (s > 0) & (s < last)
    stored = jnp.where(s == low, stored_low, stored_high)
    passed = jnp.where(s == low + 1, stored_low, stored_high)
    half = side // SPLIT
    aheads = [jnp.where((s == 1) & (odd == 0), FIRST_AHEAD, AHEAD)] + [AHEAD] * (groups - 2) + [0]
    per_group = bg * UP
    short = side // UP
    a_row = UP // 2

    load_adj = pltpu.make_async_copy(adj_hbm, adj, adj_sem)
    loads = [
        pltpu.make_async_copy(there, here, in_sem.at[n])
        for n, (there, here) in enumerate((
            (order_hbm, own_order), (x_hbm, x_ref), (order_hbm, order_ref),
            (columns_hbm, columns), (w_hbm, w_ref),
        ))
    ]
    for n in (2, 1, 0, 3, 4):
        loads[n].start()
    load_adj.start()
    barrier = pltpu.get_barrier_semaphore()

    def greet(there):
        pl.semaphore_signal(barrier, inc=1, device_id=there, device_id_type=MESH)

    peers = 2
    for neighbour in (left, right):
        greet({"dom": neighbour})
    for mask, there in (
        (s > 0, {"section": jnp.maximum(s - 1, 0)}),
        (s < last, {"section": jnp.minimum(s + 1, last)}),
    ):
        peers = peers + jnp.where(mask, 1, 0)

        @pl.when(mask)
        def _():
            greet(there)

    pl.semaphore_wait(barrier, peers)

    def order_copy(way):
        return pltpu.make_async_remote_copy(
            src_ref=order_ref,
            dst_ref=order_land.at[way],
            send_sem=order_send.at[way],
            recv_sem=order_recv.at[way],
            device_id={"dom": right if way == 0 else left},
            device_id_type=MESH,
        )

    def partner_copy(first, count, held=mine):
        return pltpu.make_async_remote_copy(
            src_ref=held.at[pl.ds(first, count)],
            dst_ref=src.at[pl.ds(to_partner + first, count)],
            send_sem=partner_send,
            recv_sem=partner_recv,
            device_id={"dom": partner},
            device_id_type=MESH,
        )

    def across_copy(n, first, count, held=mine):
        return pltpu.make_async_remote_copy(
            src_ref=held.at[pl.ds(first, count)],
            dst_ref=src.at[pl.ds(to_across + first, count)],
            send_sem=across_send.at[n],
            recv_sem=across_recv.at[n],
            device_id={"dom": across},
            device_id_type=MESH,
        )

    def relay_copy(held, landing, send, recv, there):
        return pltpu.make_async_remote_copy(
            src_ref=held, dst_ref=landing, send_sem=send, recv_sem=recv,
            device_id=there, device_id_type=MESH,
        )

    def lifts():
        return relay_copy(
            x_ref.at[pl.ds(direct, relayed)], relay_in, lift_send, lift_recv.at[0],
            {"section": low},
        )

    def crosses():
        return relay_copy(relay_in, relay_out, cross_send, cross_recv.at[0], {"dom": across})

    def downs():
        return relay_copy(
            relay_out, src.at[pl.ds(from_across + direct, relayed)], down_send, down_recv,
            {"section": 0},
        )

    def lift(b, h):
        part, q = pl.ds(h * half, half), b * SPLIT + h
        return relay_copy(
            x_ref.at[direct + b, part], relay_in.at[b, part],
            lift_send, lift_recv.at[q], {"section": low},
        )

    def cross(b, h):
        part, q = pl.ds(h * half, half), b * SPLIT + h
        return relay_copy(
            relay_in.at[b, part], relay_out.at[b, part],
            cross_send, cross_recv.at[q], {"dom": across},
        )

    def down(b, h):
        part, q = pl.ds(h * half, half), b * SPLIT + h
        return relay_copy(
            relay_out.at[b, part], src.at[from_across + direct + b, part],
            down_send, down_recv, {"section": 0},
        )

    def stored_lift(b, count):
        return relay_copy(
            mine.at[blocks - count + b], stored_in.at[b],
            slift_send, slift_recv.at[b], {"section": jnp.minimum(s + 1, last)},
        )

    def stored_cross(b):
        return relay_copy(
            stored_in.at[b], stored_out.at[b],
            scross_send, scross_recv.at[b], {"dom": across},
        )

    def stored_down(b, count):
        return relay_copy(
            stored_out.at[b], src.at[from_across + blocks - count + b],
            sdown_send, sdown_recv, {"section": jnp.maximum(s - 1, 0)},
        )

    def stored_lifts(count):
        return relay_copy(
            mine.at[pl.ds(blocks - count, count)], stored_in.at[pl.ds(0, count)],
            slift_send, slift_recv.at[0], {"section": jnp.minimum(s + 1, last)},
        )

    def stored_crosses(count):
        return relay_copy(
            stored_in.at[pl.ds(0, count)], stored_out.at[pl.ds(0, count)],
            scross_send, scross_recv.at[0], {"dom": across},
        )

    def stored_downs(count):
        return relay_copy(
            stored_out.at[pl.ds(0, count)], src.at[pl.ds(from_across + blocks - count, count)],
            sdown_send, sdown_recv, {"section": jnp.maximum(s - 1, 0)},
        )

    def up_copy(r, h):
        q = r * UP + h
        return pltpu.make_async_remote_copy(
            src_ref=out_ref.at[r, pl.ds(h * short, short)],
            dst_ref=own_land.at[q],
            send_sem=z_send.at[jnp.where(r < bg - 1, 0, 1)],
            recv_sem=z_recv.at[q],
            device_id={"section": jnp.minimum(s + 1, last)},
            device_id_type=MESH,
        )

    def up_sent(n):
        cut = (bg - 1) * UP
        part = pl.ds(0, cut) if n == 0 else pl.ds(cut, blocks * UP - cut)
        pltpu.make_async_remote_copy(
            src_ref=own_land.at[part], dst_ref=own_land.at[part],
            send_sem=z_send.at[n], recv_sem=z_recv.at[0],
            device_id={"section": jnp.minimum(s + 1, last)}, device_id_type=MESH,
        ).wait_send()

    def up_wait(q):
        pltpu.make_async_remote_copy(
            src_ref=own_land.at[q],
            dst_ref=own_land.at[q],
            send_sem=z_send.at[0],
            recv_sem=z_recv.at[q],
            device_id={"section": jnp.minimum(s + 1, last)},
            device_id_type=MESH,
        ).wait_recv()

    def side_copy(way, q):
        return pltpu.make_async_remote_copy(
            src_ref=own_land.at[q],
            dst_ref=side_land.at[way, q],
            send_sem=f_send.at[way],
            recv_sem=f_recv.at[way, q // UP],
            device_id={"dom": right if way == 0 else left},
            device_id_type=MESH,
        )

    def side_block(way, r):
        part = pl.ds(r * UP, UP)
        return pltpu.make_async_remote_copy(
            src_ref=own_land.at[part],
            dst_ref=side_land.at[way, part],
            send_sem=f_send.at[way],
            recv_sem=f_recv.at[way, r],
            device_id={"dom": right if way == 0 else left},
            device_id_type=MESH,
        )

    def side_sent(way):
        pltpu.make_async_remote_copy(
            src_ref=own_land, dst_ref=side_land.at[way],
            send_sem=f_send.at[way], recv_sem=f_recv.at[way, 0],
            device_id={"dom": right if way == 0 else left}, device_id_type=MESH,
        ).wait_send()

    def forward(q):
        up_wait(q)
        side_copy(0, q).start()
        side_copy(1, q).start()

    def stale_across(kept):
        return across_copy(0, bg, blocks - bg - kept)

    loads[2].wait()
    for way in range(2):
        order_copy(way).start()

    loads[1].wait()

    def hand_over(n):
        pl.semaphore_signal(turn.at[n], inc=1, device_id={"dom": partner}, device_id_type=MESH)

    def each_relay(step):
        @pl.loop(0, relayed)
        def _(b):
            for h in range(SPLIT):
                step(b, h)

    @pl.when((s == 0) & (odd == 0))
    def _():
        each_relay(lambda b, h: lift(b, h).start())
        across_copy(0, 0, direct, x_ref).start()

    @pl.when(s == 0)
    def _():
        partner_copy(0, blocks, x_ref).start()
        src[blocks:2 * blocks] = x_ref[...]

    loads[0].wait()

    @pl.when(s > 0)
    def _():
        for k in range(groups):
            piece = x_ref[pl.ds(own_order[0, k] * bg, bg)]
            mine[k * bg:(k + 1) * bg] = piece
            src[blocks + k * bg:blocks + (k + 1) * bg] = piece


    @pl.when(s > 0)
    def _():
        partner_copy(bg, blocks - bg).start()

    @pl.when(middle)
    def _():
        @pl.loop(0, stored)
        def _(b):
            stored_lift(b, stored).start()

    def pass_across(b, h):
        lift(b, h).wait_recv()
        cross(b, h).start()

    def pass_down(b, h):
        cross(b, h).wait_recv()
        down(b, h).start()

    @pl.when((s == low) & (odd == 0))
    def _():
        each_relay(pass_across)
        each_relay(pass_down)

    @pl.when((s == low) & (odd == 1))
    def _():
        @pl.loop(0, relayed - LAG // SPLIT)
        def _(b):
            for h in range(SPLIT):
                pass_down(b, h)

        @pl.loop(0, LAG // SPLIT)
        def _(b):
            for h in range(SPLIT):
                pass_across(b, h)
                pass_down(relayed - LAG // SPLIT + b, h)

        @pl.loop(LAG // SPLIT, relayed)
        def _(b):
            for h in range(SPLIT):
                pass_across(b, h)

    @pl.when(s == low)
    def _():
        stale_across(stored_low).start()

    @pl.when(s > low)
    def _():
        def stored_pass_across(b):
            stored_lift(b, passed).wait_recv()
            stored_cross(b).start()

        def stored_pass_down(b):
            stored_cross(b).wait_recv()
            stored_down(b, passed).start()

        stored_pass_across(0)
        stored_pass_across(1)

        @pl.loop(2, passed)
        def _(b):
            stored_pass_across(b)
            stored_pass_down(b - 2)

        @pl.when(s == last)
        def _():
            stale_across(0).start()

        @pl.when(s < last)
        def _():
            stale_across(stored_high).start()

        stored_pass_down(passed - 2)
        stored_pass_down(passed - 1)

    for way in range(2):
        order_copy(way).wait()
        local = pltpu.make_async_copy(
            order_land.at[way], near_order.at[way], order_local.at[way]
        )
        local.start()
        local.wait()

    for p in range(3):
        for g in range(groups):
            step = jnp.int32(0)
            for k in range(1, groups):
                held = own_order[0, k] if p == 1 else near_order[p // 2, 0, k]
                step = jnp.where(held == g, k, step)
            position[p * groups + g] = step

    later = s > 0
    loads[3].wait()

    @pl.loop(0, blocks)
    def _(r):
        k = r // bg
        row = own_order[0, k] * bg + r % bg
        for t in range(tiles):
            column = columns[t, row]
            relative = jnp.minimum(lax.rem(lax.div(column, blocks) - d + 1 + parts, parts), 2)
            inside = lax.rem(column, blocks)
            step = position[relative * groups + lax.div(inside, bg)]
            place = jnp.where(later, step * bg + lax.rem(inside, bg), inside)
            slot = relative * blocks + place
            table[r * tiles + t] = slot + jnp.where(later & (step <= k), fresh, 0)

    load_adj.wait()
    loads[4].wait()

    @pl.when((s == 0) & (odd == 0))
    def _():
        lifts().wait_send()
        hand_over(0)
        across_copy(0, 0, direct, x_ref).wait_send()
        hand_over(1)

    @pl.when((s == 0) & (odd == 1))
    def _():
        pl.semaphore_wait(turn.at[0], 1)
        each_relay(lambda b, h: lift(b, h).start())
        pl.semaphore_wait(turn.at[1], 1)
        across_copy(0, 0, direct, x_ref).start()

    for k in range(groups):
        lo, hi = k * bg, (k + 1) * bg
        plo, phi = lo * UP, hi * UP

        @pl.when(s > 0)
        def _():
            if k == 0:
                @pl.loop(0, per_group + aheads[0])
                def _(q):
                    forward(q)

            def as_blocks(pieces):
                return pieces.reshape(bg, side, width)

            src[fresh + blocks + lo:fresh + blocks + hi] = as_blocks(own_land[plo:phi])

            @pl.loop(lo, hi)
            def _(r):
                for way in range(2):
                    side_block(way, r).wait_recv()
                    block = side_land[way, pl.ds(r * UP, UP)]
                    src[fresh + 2 * way * blocks + r] = block.reshape(side, width)

        if k == 0:
            @pl.when(s == 0)
            def _():
                partner_copy(0, blocks, x_ref).wait_recv()
                across_copy(0, 0, direct, x_ref).wait_recv()

                downs().wait_recv()

            @pl.when(s > 0)
            def _():
                partner_copy(bg, blocks - bg).wait_recv()

            @pl.when(middle)
            def _():
                @pl.when(s == low)
                def _():
                    stale_across(stored_low).wait_recv()
                    stored_downs(stored_low).wait_recv()

                @pl.when(s > low)
                def _():
                    stale_across(stored_high).wait_recv()
                    stored_downs(stored_high).wait_recv()

            @pl.when(s == last)
            def _():
                stale_across(0).wait_recv()

        def layer_row(r):
            row = own_order[0, k] * bg + (r - lo)
            a = jnp.concatenate([adj[row, t] for t in range(tiles)], axis=1)
            h = jnp.concatenate([src[table[r * tiles + t]] for t in range(tiles)], axis=0)
            agg = jnp.dot(a, h, preferred_element_type=jnp.float32).astype(jnp.bfloat16)
            product = jnp.dot(agg, w_ref[...], preferred_element_type=jnp.float32)
            own = jnp.where(later, fresh + blocks + r, blocks + row)
            before = src[own].astype(jnp.float32)
            out_ref[r] = (before + jnp.maximum(product, 0.0)).astype(jnp.bfloat16)

        closing = (s == last) if k == groups - 1 else (s < 0)
        if k == groups - 1:
            @pl.when(closing)
            def _():
                for r in range(lo, hi):
                    layer_row(r)

        @pl.loop(lo, jnp.where(closing, lo, hi))
        def _(r):
            if k == 1:
                @pl.when((s == 0) & (odd == 1) & (r == bg + RUN))
                def _():
                    pl.semaphore_wait(turn.at[2], 1)

            layer_row(r)

            @pl.when(s < last)
            def _():
                for n in range(UP):
                    up_copy(r, n).start()

            if k + 1 < groups:
                @pl.when(s > 0)
                def _():
                    for n in range(a_row):
                        forward(phi + aheads[k] + (r - lo) * a_row + n)

        if k == 0:
            @pl.when((s == 0) & (odd == 0))
            def _():
                up_sent(0)
                hand_over(2)

        if k + 1 < groups:
            more = per_group + aheads[k + 1]

            @pl.when(s > 0)
            def _():
                @pl.loop(phi + aheads[k] + bg * a_row, phi + more)
                def _(q):
                    forward(q)

    @pl.when(s == 0)
    def _():
        partner_copy(0, blocks, x_ref).wait_send()

    @pl.when((s == 0) & (odd == 1))
    def _():
        across_copy(0, 0, direct, x_ref).wait_send()
        lifts().wait_send()

    @pl.when(s == low)
    def _():
        crosses().wait_send()
        downs().wait_send()

    @pl.when(s == low)
    def _():
        stale_across(stored_low).wait_send()
        stored_lifts(stored_low).wait_send()

    @pl.when((s > low) & (s < last))
    def _():
        stale_across(stored_high).wait_send()
        stored_lifts(stored_high).wait_send()

    @pl.when(s == last)
    def _():
        stale_across(0).wait_send()

    for mask, count in ((s == low + 1, stored_low), (s > low + 1, stored_high)):
        @pl.when(mask)
        def _():
            stored_crosses(count).wait_send()
            stored_downs(count).wait_send()

    @pl.when(s > 0)
    def _():
        partner_copy(bg, blocks - bg).wait_send()
        for way in range(2):
            side_sent(way)

    @pl.when((s < last) & ((s > 0) | (odd == 1)))
    def _():
        up_sent(0)

    @pl.when(s < last)
    def _():
        up_sent(1)


def place_kernel(groups, order, h_ref, out_hbm, out_sem):
    bg = h_ref.shape[0] // groups

    def store(k):
        return pltpu.make_async_copy(
            h_ref.at[pl.ds(k * bg, bg)], out_hbm.at[pl.ds(order[k] * bg, bg)], out_sem.at[k]
        )

    for k in range(groups):
        store(k).start()
    for k in range(groups):
        store(k).wait()


def on_device(sections, layer_inputs, adjacency, columns, group_order, weights):
    parts = lax.axis_size("dom")
    rows, width = layer_inputs.shape[1:]
    blocks, tiles, side = adjacency.shape[:3]
    groups = group_order.shape[1]
    relayed, stored, _ = relay_counts(blocks)
    pieces = blocks * UP
    dma = pltpu.SemaphoreType.DMA
    hidden = pl.pallas_call(
        functools.partial(pipeline_kernel, sections, parts, groups),
        out_shape=jax.ShapeDtypeStruct((blocks, side, width), jnp.bfloat16),
        in_specs=[
            pl.BlockSpec(memory_space=pltpu.HBM) for _ in range(5)
        ],
        out_specs=pl.BlockSpec(memory_space=pltpu.VMEM),
        scratch_shapes=[
            pltpu.SMEM((tiles, blocks), jnp.int32),
            pltpu.SMEM((1, groups), jnp.int32),
            pltpu.VMEM((1, groups), jnp.int32),
            pltpu.VMEM((blocks, side, width), jnp.bfloat16),
            pltpu.VMEM((width, width), jnp.bfloat16),
            dma((5,)),
            pltpu.SMEM((blocks * tiles,), jnp.int32),
            pltpu.SMEM((3 * groups,), jnp.int32),
            pltpu.VMEM((2, 1, groups), jnp.int32),
            pltpu.SMEM((2, 1, groups), jnp.int32),
            dma((2,)),
            dma((2,)),
            dma((2,)),
            pltpu.VMEM(adjacency.shape, jnp.bfloat16),
            pltpu.VMEM((6 * blocks, side, width), jnp.bfloat16),
            pltpu.VMEM((blocks, side, width), jnp.bfloat16),
            pltpu.VMEM((pieces, side // UP, width), jnp.bfloat16),
            pltpu.VMEM((2, pieces, side // UP, width), jnp.bfloat16),
            pltpu.VMEM((relayed, side, width), jnp.bfloat16),
            pltpu.VMEM((relayed, side, width), jnp.bfloat16),
            pltpu.VMEM((stored, side, width), jnp.bfloat16),
            pltpu.VMEM((stored, side, width), jnp.bfloat16),
            dma,
            dma,
            dma,
            dma((1,)),
            dma((1,)),
            dma((2,)),
            dma((pieces,)),
            dma((2,)),
            dma((2, blocks)),
        ] + [pltpu.SemaphoreType.REGULAR((3,))]
        + [dma, dma((relayed * SPLIT,))] * 2 + [dma, dma] + [dma, dma((stored,))] * 2 + [dma, dma],
        compiler_params=pltpu.CompilerParams(
            collective_id=0, has_side_effects=True, vmem_limit_bytes=50 * 2**20
        ),
    )(
        *(pltpu.with_memory_space_constraint(array, pltpu.HBM) for array in (
            columns.T, group_order, layer_inputs.reshape(blocks, side, width),
            adjacency, weights[0],
        ))
    )

    placed = pl.pallas_call(
        functools.partial(place_kernel, groups),
        out_shape=jax.ShapeDtypeStruct((blocks, side, width), jnp.bfloat16),
        in_specs=[
            pl.BlockSpec(memory_space=pltpu.SMEM),
            pl.BlockSpec(memory_space=pltpu.VMEM),
        ],
        out_specs=pl.BlockSpec(memory_space=pl.ANY),
        scratch_shapes=[dma((groups,))],
        compiler_params=pltpu.CompilerParams(vmem_limit_bytes=4 * 2**20),
    )(group_order[0], hidden)
    return placed.reshape(1, rows, width)


def solution(mesh):
    in_specs = (
        P("section", "dom", None),
        P("dom", None, None, None),
        P("dom", None),
        P("dom", None),
        P("section", None, None),
    )
    return jax.shard_map(
        functools.partial(on_device, mesh.shape["section"]),
        mesh=mesh, in_specs=in_specs, out_specs=P("section", "dom", None), check_vma=False,
    )
```

```python
import functools

import jax
import jax.numpy as jnp
from jax import lax
from jax.experimental import pallas as pl
from jax.experimental.pallas import tpu as pltpu
from jax.sharding import PartitionSpec as P

MESH = pl.DeviceIdType.MESH
SPLIT = 2
UP = 4
AHEAD = 3
FIRST_AHEAD = 0
RUN = 2
LAG = 4


def relay_counts(blocks):
    return blocks * 7 // 16, blocks * 5 // 8, blocks // 2


def pipeline_kernel(
    sections, parts, groups, columns_hbm, order_hbm, x_hbm, adj_hbm, w_hbm, out_ref,
    columns, own_order, order_ref, x_ref, w_ref, in_sem, table, position, order_land, near_order, order_send, order_recv, order_local,
    adj, src, mine, own_land, side_land, relay_in, relay_out, stored_in, stored_out,
    adj_sem, partner_send, partner_recv, across_send, across_recv, z_send, z_recv, f_send, f_recv,
    turn, lift_send, lift_recv, cross_send, cross_recv, down_send, down_recv,
    slift_send, slift_recv, scross_send, scross_recv, sdown_send, sdown_recv,
):
    s = lax.axis_index("section")
    d = lax.axis_index("dom")
    right, left = lax.rem(d + 1, parts), lax.rem(d + parts - 1, parts)
    blocks, side, width = x_ref.shape
    tiles = adj.shape[1]
    bg = blocks // groups
    fresh = 3 * blocks
    last = sections - 1
    odd = lax.rem(d, 2)
    partner = jnp.where(odd == 1, left, right)
    across = jnp.where(odd == 1, right, left)
    to_partner = jnp.where(odd == 1, 2 * blocks, 0)
    to_across = jnp.where(odd == 1, 0, 2 * blocks)
    from_across = jnp.where(odd == 1, 2 * blocks, 0)
    relayed, stored_low, stored_high = relay_counts(blocks)
    direct = blocks - relayed
    low = 1
    middle = (s > 0) & (s < last)
    stored = jnp.where(s == low, stored_low, stored_high)
    passed = jnp.where(s == low + 1, stored_low, stored_high)
    half = side // SPLIT
    aheads = [jnp.where((s == 1) & (odd == 0), FIRST_AHEAD, AHEAD)] + [AHEAD] * (groups - 2) + [0]
    per_group = bg * UP
    short = side // UP
    a_row = UP // 2

    load_adj = pltpu.make_async_copy(adj_hbm, adj, adj_sem)
    loads = [
        pltpu.make_async_copy(there, here, in_sem.at[n])
        for n, (there, here) in enumerate((
            (order_hbm, own_order), (x_hbm, x_ref), (order_hbm, order_ref),
            (columns_hbm, columns), (w_hbm, w_ref),
        ))
    ]
    for n in (2, 1, 0, 3, 4):
        loads[n].start()
    load_adj.start()
    barrier = pltpu.get_barrier_semaphore()

    def greet(there):
        pl.semaphore_signal(barrier, inc=1, device_id=there, device_id_type=MESH)

    peers = 2
    for neighbour in (left, right):
        greet({"dom": neighbour})
    for mask, there in (
        (s > 0, {"section": jnp.maximum(s - 1, 0)}),
        (s < last, {"section": jnp.minimum(s + 1, last)}),
    ):
        peers = peers + jnp.where(mask, 1, 0)

        @pl.when(mask)
        def _():
            greet(there)

    pl.semaphore_wait(barrier, peers)

    def order_copy(way):
        return pltpu.make_async_remote_copy(
            src_ref=order_ref,
            dst_ref=order_land.at[way],
            send_sem=order_send.at[way],
            recv_sem=order_recv.at[way],
            device_id={"dom": right if way == 0 else left},
            device_id_type=MESH,
        )

    def partner_copy(first, count, held=mine):
        return pltpu.make_async_remote_copy(
            src_ref=held.at[pl.ds(first, count)],
            dst_ref=src.at[pl.ds(to_partner + first, count)],
            send_sem=partner_send,
            recv_sem=partner_recv,
            device_id={"dom": partner},
            device_id_type=MESH,
        )

    def across_copy(n, first, count, held=mine):
        return pltpu.make_async_remote_copy(
            src_ref=held.at[pl.ds(first, count)],
            dst_ref=src.at[pl.ds(to_across + first, count)],
            send_sem=across_send.at[n],
            recv_sem=across_recv.at[n],
            device_id={"dom": across},
            device_id_type=MESH,
        )

    def relay_copy(held, landing, send, recv, there):
        return pltpu.make_async_remote_copy(
            src_ref=held, dst_ref=landing, send_sem=send, recv_sem=recv,
            device_id=there, device_id_type=MESH,
        )

    def lifts():
        return relay_copy(
            x_ref.at[pl.ds(direct, relayed)], relay_in, lift_send, lift_recv.at[0],
            {"section": low},
        )

    def crosses():
        return relay_copy(relay_in, relay_out, cross_send, cross_recv.at[0], {"dom": across})

    def downs():
        return relay_copy(
            relay_out, src.at[pl.ds(from_across + direct, relayed)], down_send, down_recv,
            {"section": 0},
        )

    def lift(b, h):
        part, q = pl.ds(h * half, half), b * SPLIT + h
        return relay_copy(
            x_ref.at[direct + b, part], relay_in.at[b, part],
            lift_send, lift_recv.at[q], {"section": low},
        )

    def cross(b, h):
        part, q = pl.ds(h * half, half), b * SPLIT + h
        return relay_copy(
            relay_in.at[b, part], relay_out.at[b, part],
            cross_send, cross_recv.at[q], {"dom": across},
        )

    def down(b, h):
        part, q = pl.ds(h * half, half), b * SPLIT + h
        return relay_copy(
            relay_out.at[b, part], src.at[from_across + direct + b, part],
            down_send, down_recv, {"section": 0},
        )

    def stored_lift(b, count):
        return relay_copy(
            mine.at[blocks - count + b], stored_in.at[b],
            slift_send, slift_recv.at[b], {"section": jnp.minimum(s + 1, last)},
        )

    def stored_cross(b):
        return relay_copy(
            stored_in.at[b], stored_out.at[b],
            scross_send, scross_recv.at[b], {"dom": across},
        )

    def stored_down(b, count):
        return relay_copy(
            stored_out.at[b], src.at[from_across + blocks - count + b],
            sdown_send, sdown_recv, {"section": jnp.maximum(s - 1, 0)},
        )

    def stored_lifts(count):
        return relay_copy(
            mine.at[pl.ds(blocks - count, count)], stored_in.at[pl.ds(0, count)],
            slift_send, slift_recv.at[0], {"section": jnp.minimum(s + 1, last)},
        )

    def stored_crosses(count):
        return relay_copy(
            stored_in.at[pl.ds(0, count)], stored_out.at[pl.ds(0, count)],
            scross_send, scross_recv.at[0], {"dom": across},
        )

    def stored_downs(count):
        return relay_copy(
            stored_out.at[pl.ds(0, count)], src.at[pl.ds(from_across + blocks - count, count)],
            sdown_send, sdown_recv, {"section": jnp.maximum(s - 1, 0)},
        )

    def up_copy(r, h):
        q = r * UP + h
        return pltpu.make_async_remote_copy(
            src_ref=out_ref.at[r, pl.ds(h * short, short)],
            dst_ref=own_land.at[q],
            send_sem=z_send.at[jnp.where(r < bg - 1, 0, 1)],
            recv_sem=z_recv.at[q],
            device_id={"section": jnp.minimum(s + 1, last)},
            device_id_type=MESH,
        )

    def up_sent(n):
        cut = (bg - 1) * UP
        part = pl.ds(0, cut) if n == 0 else pl.ds(cut, blocks * UP - cut)
        pltpu.make_async_remote_copy(
            src_ref=own_land.at[part], dst_ref=own_land.at[part],
            send_sem=z_send.at[n], recv_sem=z_recv.at[0],
            device_id={"section": jnp.minimum(s + 1, last)}, device_id_type=MESH,
        ).wait_send()

    def up_wait(q):
        pltpu.make_async_remote_copy(
            src_ref=own_land.at[q],
            dst_ref=own_land.at[q],
            send_sem=z_send.at[0],
            recv_sem=z_recv.at[q],
            device_id={"section": jnp.minimum(s + 1, last)},
            device_id_type=MESH,
        ).wait_recv()

    def side_copy(way, q):
        return pltpu.make_async_remote_copy(
            src_ref=own_land.at[q],
            dst_ref=side_land.at[way, q],
            send_sem=f_send.at[way],
            recv_sem=f_recv.at[way, q // UP],
            device_id={"dom": right if way == 0 else left},
            device_id_type=MESH,
        )

    def side_block(way, r):
        part = pl.ds(r * UP, UP)
        return pltpu.make_async_remote_copy(
            src_ref=own_land.at[part],
            dst_ref=side_land.at[way, part],
            send_sem=f_send.at[way],
            recv_sem=f_recv.at[way, r],
            device_id={"dom": right if way == 0 else left},
            device_id_type=MESH,
        )

    def side_sent(way):
        pltpu.make_async_remote_copy(
            src_ref=own_land, dst_ref=side_land.at[way],
            send_sem=f_send.at[way], recv_sem=f_recv.at[way, 0],
            device_id={"dom": right if way == 0 else left}, device_id_type=MESH,
        ).wait_send()

    def forward(q):
        up_wait(q)
        side_copy(0, q).start()
        side_copy(1, q).start()

    def stale_across(kept):
        return across_copy(0, bg, blocks - bg - kept)

    loads[2].wait()
    for way in range(2):
        order_copy(way).start()

    loads[1].wait()

    def hand_over(n):
        pl.semaphore_signal(turn.at[n], inc=1, device_id={"dom": partner}, device_id_type=MESH)

    def each_relay(step):
        @pl.loop(0, relayed)
        def _(b):
            for h in range(SPLIT):
                step(b, h)

    @pl.when((s == 0) & (odd == 0))
    def _():
        each_relay(lambda b, h: lift(b, h).start())
        across_copy(0, 0, direct, x_ref).start()

    @pl.when(s == 0)
    def _():
        partner_copy(0, blocks, x_ref).start()
        src[blocks:2 * blocks] = x_ref[...]

    loads[0].wait()

    @pl.when(s > 0)
    def _():
        for k in range(groups):
            piece = x_ref[pl.ds(own_order[0, k] * bg, bg)]
            mine[k * bg:(k + 1) * bg] = piece
            src[blocks + k * bg:blocks + (k + 1) * bg] = piece


    @pl.when(s > 0)
    def _():
        partner_copy(bg, blocks - bg).start()

    @pl.when(middle)
    def _():
        @pl.loop(0, stored)
        def _(b):
            stored_lift(b, stored).start()

    def pass_across(b, h):
        lift(b, h).wait_recv()
        cross(b, h).start()

    def pass_down(b, h):
        cross(b, h).wait_recv()
        down(b, h).start()

    @pl.when((s == low) & (odd == 0))
    def _():
        each_relay(pass_across)
        each_relay(pass_down)

    @pl.when((s == low) & (odd == 1))
    def _():
        @pl.loop(0, relayed - LAG // SPLIT)
        def _(b):
            for h in range(SPLIT):
                pass_down(b, h)

        @pl.loop(0, LAG // SPLIT)
        def _(b):
            for h in range(SPLIT):
                pass_across(b, h)
                pass_down(relayed - LAG // SPLIT + b, h)

        @pl.loop(LAG // SPLIT, relayed)
        def _(b):
            for h in range(SPLIT):
                pass_across(b, h)

    @pl.when(s == low)
    def _():
        stale_across(stored_low).start()

    @pl.when(s > low)
    def _():
        def stored_pass_across(b):
            stored_lift(b, passed).wait_recv()
            stored_cross(b).start()

        def stored_pass_down(b):
            stored_cross(b).wait_recv()
            stored_down(b, passed).start()

        stored_pass_across(0)
        stored_pass_across(1)

        @pl.loop(2, passed)
        def _(b):
            stored_pass_across(b)
            stored_pass_down(b - 2)

        @pl.when(s == last)
        def _():
            stale_across(0).start()

        @pl.when(s < last)
        def _():
            stale_across(stored_high).start()

        stored_pass_down(passed - 2)
        stored_pass_down(passed - 1)

    for way in range(2):
        order_copy(way).wait()
        local = pltpu.make_async_copy(
            order_land.at[way], near_order.at[way], order_local.at[way]
        )
        local.start()
        local.wait()

    for p in range(3):
        for g in range(groups):
            step = jnp.int32(0)
            for k in range(1, groups):
                held = own_order[0, k] if p == 1 else near_order[p // 2, 0, k]
                step = jnp.where(held == g, k, step)
            position[p * groups + g] = step

    later = s > 0
    loads[3].wait()

    @pl.loop(0, blocks)
    def _(r):
        k = r // bg
        row = own_order[0, k] * bg + r % bg
        for t in range(tiles):
            column = columns[t, row]
            relative = jnp.minimum(lax.rem(lax.div(column, blocks) - d + 1 + parts, parts), 2)
            inside = lax.rem(column, blocks)
            step = position[relative * groups + lax.div(inside, bg)]
            place = jnp.where(later, step * bg + lax.rem(inside, bg), inside)
            slot = relative * blocks + place
            table[r * tiles + t] = slot + jnp.where(later & (step <= k), fresh, 0)

    load_adj.wait()
    loads[4].wait()

    @pl.when((s == 0) & (odd == 0))
    def _():
        lifts().wait_send()
        hand_over(0)
        across_copy(0, 0, direct, x_ref).wait_send()
        hand_over(1)

    @pl.when((s == 0) & (odd == 1))
    def _():
        pl.semaphore_wait(turn.at[0], 1)
        each_relay(lambda b, h: lift(b, h).start())
        pl.semaphore_wait(turn.at[1], 1)
        across_copy(0, 0, direct, x_ref).start()

    for k in range(groups):
        lo, hi = k * bg, (k + 1) * bg
        plo, phi = lo * UP, hi * UP

        @pl.when(s > 0)
        def _():
            if k == 0:
                @pl.loop(0, per_group + aheads[0])
                def _(q):
                    forward(q)

            def as_blocks(pieces):
                return pieces.reshape(bg, side, width)

            src[fresh + blocks + lo:fresh + blocks + hi] = as_blocks(own_land[plo:phi])

            @pl.loop(lo, hi)
            def _(r):
                for way in range(2):
                    side_block(way, r).wait_recv()
                    block = side_land[way, pl.ds(r * UP, UP)]
                    src[fresh + 2 * way * blocks + r] = block.reshape(side, width)

        if k == 0:
            @pl.when(s == 0)
            def _():
                partner_copy(0, blocks, x_ref).wait_recv()
                across_copy(0, 0, direct, x_ref).wait_recv()

                downs().wait_recv()

            @pl.when(s > 0)
            def _():
                partner_copy(bg, blocks - bg).wait_recv()

            @pl.when(middle)
            def _():
                @pl.when(s == low)
                def _():
                    stale_across(stored_low).wait_recv()
                    stored_downs(stored_low).wait_recv()

                @pl.when(s > low)
                def _():
                    stale_across(stored_high).wait_recv()
                    stored_downs(stored_high).wait_recv()

            @pl.when(s == last)
            def _():
                stale_across(0).wait_recv()

        def layer_row(r):
            row = own_order[0, k] * bg + (r - lo)
            a = jnp.concatenate([adj[row, t] for t in range(tiles)], axis=1)
            h = jnp.concatenate([src[table[r * tiles + t]] for t in range(tiles)], axis=0)
            agg = jnp.dot(a, h, preferred_element_type=jnp.float32).astype(jnp.bfloat16)
            product = jnp.dot(agg, w_ref[...], preferred_element_type=jnp.float32)
            own = jnp.where(later, fresh + blocks + r, blocks + row)
            before = src[own].astype(jnp.float32)
            out_ref[r] = (before + jnp.maximum(product, 0.0)).astype(jnp.bfloat16)

        closing = (s == last) if k == groups - 1 else (s < 0)
        if k == groups - 1:
            @pl.when(closing)
            def _():
                for r in range(lo, hi):
                    layer_row(r)

        @pl.loop(lo, jnp.where(closing, lo, hi))
        def _(r):
            if k == 1:
                @pl.when((s == 0) & (odd == 1) & (r == bg + RUN))
                def _():
                    pl.semaphore_wait(turn.at[2], 1)

            layer_row(r)

            @pl.when(s < last)
            def _():
                for n in range(UP):
                    up_copy(r, n).start()

            if k + 1 < groups:
                @pl.when(s > 0)
                def _():
                    for n in range(a_row):
                        forward(phi + aheads[k] + (r - lo) * a_row + n)

        if k == 0:
            @pl.when((s == 0) & (odd == 0))
            def _():
                up_sent(0)
                hand_over(2)

        if k + 1 < groups:
            more = per_group + aheads[k + 1]

            @pl.when(s > 0)
            def _():
                @pl.loop(phi + aheads[k] + bg * a_row, phi + more)
                def _(q):
                    forward(q)

    @pl.when(s == 0)
    def _():
        partner_copy(0, blocks, x_ref).wait_send()

    @pl.when((s == 0) & (odd == 1))
    def _():
        across_copy(0, 0, direct, x_ref).wait_send()
        lifts().wait_send()

    @pl.when(s == low)
    def _():
        crosses().wait_send()
        downs().wait_send()

    @pl.when(s == low)
    def _():
        stale_across(stored_low).wait_send()
        stored_lifts(stored_low).wait_send()

    @pl.when((s > low) & (s < last))
    def _():
        stale_across(stored_high).wait_send()
        stored_lifts(stored_high).wait_send()

    @pl.when(s == last)
    def _():
        stale_across(0).wait_send()

    for mask, count in ((s == low + 1, stored_low), (s > low + 1, stored_high)):
        @pl.when(mask)
        def _():
            stored_crosses(count).wait_send()
            stored_downs(count).wait_send()

    @pl.when(s > 0)
    def _():
        partner_copy(bg, blocks - bg).wait_send()
        for way in range(2):
            side_sent(way)

    @pl.when((s < last) & ((s > 0) | (odd == 1)))
    def _():
        up_sent(0)

    @pl.when(s < last)
    def _():
        up_sent(1)


def place_kernel(groups, order, h_ref, out_hbm, out_sem):
    bg = h_ref.shape[0] // groups

    def store(k):
        return pltpu.make_async_copy(
            h_ref.at[pl.ds(k * bg, bg)], out_hbm.at[pl.ds(order[k] * bg, bg)], out_sem.at[k]
        )

    for k in range(groups):
        store(k).start()
    for k in range(groups):
        store(k).wait()


def on_device(sections, layer_inputs, adjacency, columns, group_order, weights):
    parts = lax.axis_size("dom")
    rows, width = layer_inputs.shape[1:]
    blocks, tiles, side = adjacency.shape[:3]
    groups = group_order.shape[1]
    relayed, stored, _ = relay_counts(blocks)
    pieces = blocks * UP
    dma = pltpu.SemaphoreType.DMA
    hidden = pl.pallas_call(
        functools.partial(pipeline_kernel, sections, parts, groups),
        out_shape=jax.ShapeDtypeStruct((blocks, side, width), jnp.bfloat16),
        in_specs=[
            pl.BlockSpec(memory_space=pltpu.HBM) for _ in range(5)
        ],
        out_specs=pl.BlockSpec(memory_space=pltpu.VMEM),
        scratch_shapes=[
            pltpu.SMEM((tiles, blocks), jnp.int32),
            pltpu.SMEM((1, groups), jnp.int32),
            pltpu.VMEM((1, groups), jnp.int32),
            pltpu.VMEM((blocks, side, width), jnp.bfloat16),
            pltpu.VMEM((width, width), jnp.bfloat16),
            dma((5,)),
            pltpu.SMEM((blocks * tiles,), jnp.int32),
            pltpu.SMEM((3 * groups,), jnp.int32),
            pltpu.VMEM((2, 1, groups), jnp.int32),
            pltpu.SMEM((2, 1, groups), jnp.int32),
            dma((2,)),
            dma((2,)),
            dma((2,)),
            pltpu.VMEM(adjacency.shape, jnp.bfloat16),
            pltpu.VMEM((6 * blocks, side, width), jnp.bfloat16),
            pltpu.VMEM((blocks, side, width), jnp.bfloat16),
            pltpu.VMEM((pieces, side // UP, width), jnp.bfloat16),
            pltpu.VMEM((2, pieces, side // UP, width), jnp.bfloat16),
            pltpu.VMEM((relayed, side, width), jnp.bfloat16),
            pltpu.VMEM((relayed, side, width), jnp.bfloat16),
            pltpu.VMEM((stored, side, width), jnp.bfloat16),
            pltpu.VMEM((stored, side, width), jnp.bfloat16),
            dma,
            dma,
            dma,
            dma((1,)),
            dma((1,)),
            dma((2,)),
            dma((pieces,)),
            dma((2,)),
            dma((2, blocks)),
        ] + [pltpu.SemaphoreType.REGULAR((3,))]
        + [dma, dma((relayed * SPLIT,))] * 2 + [dma, dma] + [dma, dma((stored,))] * 2 + [dma, dma],
        compiler_params=pltpu.CompilerParams(
            collective_id=0, has_side_effects=True, vmem_limit_bytes=50 * 2**20
        ),
    )(
        *(pltpu.with_memory_space_constraint(array, pltpu.HBM) for array in (
            columns.T, group_order, layer_inputs.reshape(blocks, side, width),
            adjacency, weights[0],
        ))
    )

    placed = pl.pallas_call(
        functools.partial(place_kernel, groups),
        out_shape=jax.ShapeDtypeStruct((blocks, side, width), jnp.bfloat16),
        in_specs=[
            pl.BlockSpec(memory_space=pltpu.SMEM),
            pl.BlockSpec(memory_space=pltpu.VMEM),
        ],
        out_specs=pl.BlockSpec(memory_space=pl.ANY),
        scratch_shapes=[dma((groups,))],
        compiler_params=pltpu.CompilerParams(vmem_limit_bytes=4 * 2**20),
    )(group_order[0], hidden)
    return placed.reshape(1, rows, width)


def solution(mesh):
    in_specs = (
        P("section", "dom", None),
        P("dom", None, None, None),
        P("dom", None),
        P("dom", None),
        P("section", None, None),
    )
    return jax.shard_map(
        functools.partial(on_device, mesh.shape["section"]),
        mesh=mesh, in_specs=in_specs, out_specs=P("section", "dom", None), check_vma=False,
    )
```
